256 devices in a mesh: seq: 32 (over y, z), head: 8 (over x, core).
Axes of the slice: x: 4, y: 4, z: 8, core: 2. Of those that a mesh axis runs over, the one named last changes fastest.
Arguments:
- queries: float32 [4096, 32, 128], P('seq', 'head'), may hold values from -0.6 to 0.6
- keys: float32 [4096, 32, 128], P('seq', 'head'), may hold values from -0.6 to 0.6
- values: float32 [4096, 32, 128], P('seq', 'head'), may hold values from -6 to 6
- level_weights: float32 [7, 32, 4096], P(None, 'head', 'seq'), may hold values from 0.02 to 0.2
- out_proj: bfloat16 [4096, 4096], P('head'), may hold values from -0.125 to 0.125
- out_grad: bfloat16 [4096, 4096], P('seq', 'head'), may hold values from -6 to 6
Outputs:
- mixed: bfloat16 [4096, 4096], P('seq', 'head')
- query_grad: float32 [4096, 32, 128], P('seq', 'head')
- key_grad: float32 [4096, 32, 128], P('seq', 'head')
- value_grad: float32 [4096, 32, 128], P('seq', 'head')
- proj_grad: float32 [4096, 4096], P('head', 'seq')
The draws below stay inside these ranges and needn't reach their ends.
All inputs are finite; a program needn't handle non-finite values.
Results may differ from the reference program's by a relative error of at most 0.015.
Values may be sent and summed in bfloat16 or wider, within the bound.
A program may use at most 64 MiB of HBM per device.

```python
import math
import jax
import jax.numpy as jnp
from jax import lax

D = 4096
HEADS = 32
HD = 128
CH = 64
TOKENS = 4096
LOCAL_BITS = 1
SEQ_BITS = 5
LEVELS = 7


def with_spikes(entries, stream_key, source, target, parts, factor):
    def block_of(axis_at):
        return (jnp.arange(entries.shape[axis_at]) // (entries.shape[axis_at] // parts)).reshape((-1,) + (1,) * (entries.ndim - 1 - axis_at))

    one_side = jax.random.permutation(stream_key, parts)[block_of(target)]
    second = (block_of(target) + parts // 2) % parts
    return jnp.where((block_of(source) == one_side) | (block_of(source) == second), factor * entries, entries)


def steps_of(key, dims, shards, least, top_value):
    def one(axis_at, blocks):
        steps = jax.random.uniform(jax.random.fold_in(jax.random.fold_in(key, 6), axis_at), (blocks,), jnp.float32, least / len(shards), top_value / len(shards))
        return jnp.repeat(jnp.exp(steps), dims[axis_at] // blocks).reshape((-1,) + (1,) * (len(dims) - axis_at - 1))

    factor_of = one(*shards[0])
    for cut in shards[1:]:
        factor_of = factor_of * one(*cut)
    return factor_of


def gaussian(key, shape, deviation, limit, pieces=(), held_as=jnp.bfloat16):
    loudness = steps_of(key, shape, pieces, -0.22, 0.18) if pieces else 1.0
    entries = jax.random.normal(key, shape, jnp.float32) * deviation * loudness
    return jnp.minimum(jnp.maximum(entries, -limit), limit).astype(held_as)


def heavy_noise(rng, dims, spread, bound, split, heavy, kind=jnp.bfloat16):
    array = spread * jax.random.normal(rng, dims, jnp.float32)
    if split:
        array = array * steps_of(rng, dims, split, -0.22, 0.18)
    return jnp.clip(with_spikes(array, jax.random.fold_in(rng, 3), *heavy), -bound, bound).astype(kind)


def setup_inputs(seed: int = 0) -> dict:
    streams_of = jax.random.split(jax.random.key(seed), 7)
    return {
        "queries": gaussian(streams_of[0], (TOKENS, HEADS, HD), 0.1, 0.6, ((0, 32), (1, 8)), jnp.float32),
        "keys": gaussian(streams_of[1], (TOKENS, HEADS, HD), 0.1, 0.6, ((0, 32), (1, 8)), jnp.float32),
        "values": gaussian(streams_of[2], (TOKENS, HEADS, HD), 1.0, 6.0, ((0, 32), (1, 8)), jnp.float32),
        "level_weights": jnp.clip(jnp.exp(math.log(0.2) - 2.3025851 * jax.random.uniform(streams_of[3], (LEVELS, HEADS, TOKENS), jnp.float32) ** steps_of(streams_of[3], (LEVELS, HEADS, TOKENS), ((1, 8), (2, 32)), -0.2, 0.2)), 0.02, 0.2),
        "out_proj": heavy_noise(streams_of[4], (D, D), D ** -0.5, 0.125, ((0, 8),), (0, 1, 8, 2.0)),
        "out_grad": heavy_noise(streams_of[5], (TOKENS, D), 1.0, 6.0, ((0, 32), (1, 8)), (0, 1, 32, 2.75)),
    }


def head_pass(qh, kh, vh, lamh, gh):
    hp = lax.Precision.HIGHEST
    total, hdim = qh.shape
    nchunk = total // CH
    qc = qh.reshape(nchunk, CH, hdim)
    kc = kh.reshape(nchunk, CH, hdim)
    vc = vh.reshape(nchunk, CH, hdim)
    gc = gh.reshape(nchunk, CH, hdim)
    causal = (jnp.arange(CH)[:, None] >= jnp.arange(CH)[None, :]).astype(jnp.float32)
    weight = lamh[0].reshape(nchunk, CH)[:, :, None] * causal
    scores = jnp.einsum('csd,crd->csr', qc, kc, precision=hp)
    probs = scores * weight
    out = jnp.einsum('csr,crd->csd', probs, vc, precision=hp).reshape(total, hdim)
    dprobs = jnp.einsum('csd,crd->csr', gc, vc, precision=hp) * weight
    dq = jnp.einsum('csr,crd->csd', dprobs, kc, precision=hp).reshape(total, hdim)
    dk = jnp.einsum('csr,csd->crd', dprobs, qc, precision=hp).reshape(total, hdim)
    dv = jnp.einsum('csr,csd->crd', probs, gc, precision=hp).reshape(total, hdim)
    for bit in range(LOCAL_BITS + SEQ_BITS):
        span = CH * 2 ** bit
        groups = total // (2 * span)
        q2 = qh.reshape(groups, 2, span, hdim)
        k2 = kh.reshape(groups, 2, span, hdim)
        v2 = vh.reshape(groups, 2, span, hdim)
        g2 = gh.reshape(groups, 2, span, hdim)
        lam2 = lamh[1 + bit].reshape(groups, 2, span)[:, 1, :, None]
        state = jnp.einsum('nrd,nre->nde', k2[:, 0], v2[:, 0], precision=hp)
        grads = jnp.einsum('nrd,nre->nde', lam2 * q2[:, 1], g2[:, 1], precision=hp)
        zero = jnp.zeros((groups, span, hdim), jnp.float32)
        out_inc = lam2 * jnp.einsum('nrd,nde->nre', q2[:, 1], state, precision=hp)
        dq_inc = lam2 * jnp.einsum('nre,nde->nrd', g2[:, 1], state, precision=hp)
        dk_inc = jnp.einsum('nre,nde->nrd', v2[:, 0], grads, precision=hp)
        dv_inc = jnp.einsum('nrd,nde->nre', k2[:, 0], grads, precision=hp)
        out = out + jnp.stack([zero, out_inc], axis=1).reshape(total, hdim)
        dq = dq + jnp.stack([zero, dq_inc], axis=1).reshape(total, hdim)
        dk = dk + jnp.stack([dk_inc, zero], axis=1).reshape(total, hdim)
        dv = dv + jnp.stack([dv_inc, zero], axis=1).reshape(total, hdim)
    return out, dq, dk, dv


def reference(queries, keys, values, level_weights, out_proj, out_grad):
    total, heads, hdim = queries.shape
    grad_heads = jnp.dot(out_grad, out_proj.T, preferred_element_type=jnp.float32).reshape(total, heads, hdim)

    def one_head(index):
        return head_pass(queries[:, index], keys[:, index], values[:, index], level_weights[:, index], grad_heads[:, index])

    out, dq, dk, dv = lax.map(one_head, jnp.arange(heads, dtype=jnp.int32))
    attended = jnp.transpose(out, (1, 0, 2)).reshape(total, heads * hdim).astype(jnp.bfloat16)
    mixed = jnp.dot(attended, out_proj, preferred_element_type=jnp.float32).astype(jnp.bfloat16)
    proj_grad = jnp.dot(attended.T, out_grad, preferred_element_type=jnp.float32)
    return (mixed, jnp.transpose(dq, (1, 0, 2)), jnp.transpose(dk, (1, 0, 2)), jnp.transpose(dv, (1, 0, 2)), proj_grad)
```

```python
import functools

import jax
import jax.numpy as jnp
from jax import lax
from jax.experimental import pallas as pl
from jax.experimental.pallas import tpu as pltpu
from jax.sharding import PartitionSpec as P

MESH = pl.DeviceIdType.MESH
BF = jnp.bfloat16
F32 = jnp.float32
NN = (((1,), (0,)), ((), ()))
NT = (((1,), (1,)), ((), ()))
TN = (((0,), (0,)), ((), ()))
NY, NZ, NX = 4, 8, 4
HH = 4
HALF = 256


def mm(a, b, dims=NN):
    return lax.dot_general(a, b, dims, preferred_element_type=F32)


class Ids:
    def __init__(self):
        self.table = {}

    def __call__(self, *key):
        return self.table.setdefault(key, len(self.table))


def body_kernel(
    q_h, k_h, v_h, lam_h, wo_h, og_h,
    mixed_o, dq_o, dk_o, dv_o, pg_o,
    qf, kf, vf, lam_v, lam_s, lam_t, wo, gf, gacc,
    qb, kb, vb, gb, pb, db, attf, att16,
    sb, st, sty, tsend, trecv, s34, urecv, uacc,
    du, dd, ru, rd, dn,
    bb, at, cf, cu, cd, xu, xd,
    mp, mr, ms, mx,
    dqv, dkv, dvv, pgv, mixv,
    lsem, ssem, rsem,
):
    seq = lax.axis_index("seq")
    hd = lax.axis_index("head")
    y, z = lax.div(seq, NZ), lax.rem(seq, NZ)
    x, c = lax.div(hd, 2), lax.rem(hd, 2)
    sib = 1 - c

    def dev(yy, zz, xx, cc):
        return (yy * NZ + zz, xx * 2 + cc)

    def up(j):
        return lax.rem(z + j + NZ, NZ)

    def yp(j):
        return lax.rem(y + j + NY, NY)

    def xp(j):
        return lax.rem(x + j + NX, NX)

    d_sib = dev(y, z, x, sib)
    d_x = {j: dev(y, z, xp(j), c) for j in (1, 2, 3)}
    d_y = {j: dev(yp(j), z, x, c) for j in (1, 2, 3)}
    d_up, d_dn = dev(y, up(1), x, c), dev(y, up(-1), x, c)

    ids = Ids()
    pending = []

    def rcopy(src, dst, i, device):
        return pltpu.make_async_remote_copy(
            src_ref=src, dst_ref=dst, send_sem=ssem.at[i], recv_sem=rsem.at[i],
            device_id=device, device_id_type=MESH,
        )

    def send(src, dst, key, device):
        op = rcopy(src, dst, ids(*key), device)
        op.start()
        pending.append(op)

    def recv(dst, key, device):
        rcopy(dst, dst, ids(*key), device).wait_recv()

    loads = {}

    def load(name, src, dst):
        op = pltpu.make_async_copy(src, dst, lsem.at[len(loads)])
        op.start()
        loads[name] = op

    load("k", k_h, kf)
    load("v", v_h, vf)
    load("og", og_h, gf.at[hd])
    load("q", q_h, qf)
    load("lam", lam_h, lam_v)
    load("wo", wo_h, wo)

    barrier = pltpu.get_barrier_semaphore()
    partners = [d_sib] + [d_x[j] for j in (1, 2, 3)] + [d_y[j] for j in (1, 2, 3)] + [d_up, d_dn]
    for who in partners:
        pl.semaphore_signal(barrier, inc=1, device_id=who, device_id_type=MESH)
    pl.semaphore_wait(barrier, len(partners))

    for j in (2, 1, 3):
        send(og_h, gf.at[hd], ("og", j), d_x[j])
    send(og_h, gf.at[hd], ("og", 0), d_sib)

    loads["k"].wait()
    loads["v"].wait()

    def rows(ref, h):
        return ref[pl.ds(h, 128, stride=HH), :]

    for h in range(HH):
        kh = rows(kf, h).astype(BF)
        vh = rows(vf, h).astype(BF)
        kb[h] = kh
        vb[h] = vh
        sb[z, pl.ds(128 * h, 128), :] = mm(kh, vh, TN).astype(BF)

    def half(i):
        return pl.ds(HALF * i, HALF)

    def ag_send(k):
        su, sd = up(-k), up(k)
        for i in (0, 1):
            if k < 3 or i == 0:
                send(sb.at[su, half(i)], sb.at[su, half(i)], ("agu", k, i), d_up)
            if k < 3 or i == 1:
                send(sb.at[sd, half(i)], sb.at[sd, half(i)], ("agd", k, i), d_dn)

    def ag_recv(k, i, dirs=("u", "d")):
        if "u" in dirs:
            recv(sb.at[up(-k - 1), half(i)], ("agu", k, i), d_up)
        if "d" in dirs:
            recv(sb.at[up(k + 1), half(i)], ("agd", k, i), d_dn)

    def ag_relay(k):
        su, sd = up(-k), up(k)
        for i in (0, 1):
            ag_recv(k - 1, i)
            if k < 3 or i == 0:
                send(sb.at[su, half(i)], sb.at[su, half(i)], ("agu", k, i), d_up)
            if k < 3 or i == 1:
                send(sb.at[sd, half(i)], sb.at[sd, half(i)], ("agd", k, i), d_dn)

    ag_send(0)

    loads["q"].wait()
    loads["lam"].wait()
    lam_s[...] = jnp.zeros_like(lam_s)
    for l in range(7):
        lam_s[pl.ds(4 * l, 4), :] = lam_v[l]
    lam_t[...] = lam_s[...].T

    def lam(l, h):
        return lam_t[:, 4 * l + h : 4 * l + h + 1]

    t_pos = lax.broadcasted_iota(jnp.int32, (128, 128), 0)
    s_pos = lax.broadcasted_iota(jnp.int32, (128, 128), 1)
    causal = t_pos >= s_pos
    cross = (t_pos >= 64) & (s_pos < 64)

    def weight(h):
        return jnp.where(causal, jnp.where(cross, lam(1, h), lam(0, h)), 0.0)

    for h in range(HH):
        qh = rows(qf, h).astype(BF)
        qb[h] = qh
        probs = (mm(qh, kb[h], NT) * weight(h)).astype(BF)
        pb[h] = probs
        attf[h] = mm(probs, vb[h])

    ag_relay(1)

    loads["og"].wait()
    loads["wo"].wait()

    def g_part(index):
        cols = pl.ds(pl.multiple_of(index * 512, 512), 512)
        return mm(gf[index], wo[:, cols], NT)

    gacc[...] = g_part(hd)
    for j in (1, 3, 2):
        src = xp(-j) * 2 + c
        recv(gf.at[src], ("og", j), d_x[j])
        send(gf.at[src], gf.at[src], ("og2", j), d_sib)
    for j in (1, 2, 3):
        send(gf.at[yp(j) * 2 + c], bb.at[y, c], ("b", j), d_y[j])
    ag_relay(2)
    for j in (1, 3, 2):
        gacc[...] += g_part(xp(-j) * 2 + c)
    recv(gf.at[x * 2 + sib], ("og", 0), d_sib)
    gacc[...] += g_part(x * 2 + sib)
    for j in (1, 3, 2):
        src = xp(-j) * 2 + sib
        recv(gf.at[src], ("og2", j), d_sib)
        gacc[...] += g_part(src)
    for h in range(HH):
        gb[h] = gacc[:, 128 * h : 128 * h + 128].astype(BF)
    for i in (0, 1):
        bb[y, i] = gf[y * 2 + i]

    ag_relay(3)

    def weighted(h, level):
        return (qb[h].astype(F32) * lam(level, h)).astype(BF)

    for d in (4, 3):
        for h in range(HH):
            sty[d - 3, pl.ds(128 * h, 128), :] = mm(weighted(h, 2 + d), gb[h], TN).astype(BF)
    near = lax.rem(y, 2)
    for j in (1, 2, 3):

        @pl.when(y >= j)
        def _(j=j):
            which = 1 - near if j == 1 else 1
            rcopy(sty.at[which], urecv.at[j - 1], ids("u", j), d_y[4 - j]).start()

    for d in (0, 1, 2):
        for h in range(HH):
            st[d, pl.ds(128 * h, 128), :] = mm(weighted(h, 2 + d), gb[h], TN)

    for h in range(HH):
        db[h] = (mm(gb[h], vb[h], NT) * weight(h)).astype(BF)
        dqv[pl.ds(h, 128, stride=HH), :] = mm(db[h], kb[h])
        dkv[pl.ds(h, 128, stride=HH), :] = mm(db[h], qb[h], TN)
        dvv[pl.ds(h, 128, stride=HH), :] = mm(pb[h], gb[h], TN)

    ag_recv(3, 0, "u")
    ag_recv(3, 1, "d")
    z1 = z + 1 - 2 * lax.rem(z, 2)
    zp = lax.div(z, 2)
    zp1 = 2 * (zp + 1 - 2 * lax.rem(zp, 2))
    zq1 = 4 * (1 - lax.div(z, 4))
    total = sb[0].astype(F32)
    for i in range(1, NZ):
        total = total + sb[i].astype(F32)
    tsend[...] = total.astype(BF)
    for j in (1, 2, 3):

        @pl.when(y + j < NY)
        def _(j=j):
            rcopy(tsend, trecv.at[j - 1], ids("t", j), d_y[j]).start()

    pair = (sb[zp1].astype(F32) + sb[zp1 + 1].astype(F32)).astype(BF)
    quad = sb[zq1].astype(F32)
    for i in range(1, 4):
        quad = quad + sb[zq1 + i].astype(F32)
    quad = quad.astype(BF)
    single = sb[z1]
    b0 = lax.rem(z, 2).astype(F32)
    b1 = lax.rem(zp, 2).astype(F32)
    b2 = lax.div(z, 4).astype(F32)

    def from_states(states, levels, bits):
        for h in range(HH):
            block = jnp.concatenate([s[128 * h : 128 * h + 128] for s in states], axis=0)
            wide = jnp.concatenate([s[128 * h : 128 * h + 128] for s in states], axis=1)
            qw, gw = [], []
            for l, bit in zip(levels, bits):
                scale = lam(l, h) if bit is None else lam(l, h) * bit
                qw.append((qb[h].astype(F32) * scale).astype(BF))
                gw.append((gb[h].astype(F32) * scale).astype(BF))
            attf[h] += mm(jnp.concatenate(qw, axis=1), block)
            place = pl.ds(h, 128, stride=HH)
            dqv[place, :] = dqv[place, :] + mm(jnp.concatenate(gw, axis=1), wide, NT)

    from_states([single, pair, quad], (2, 3, 4), (b0, b1, b2))

    def rs_step(k, own, bu, bd, pu, pd, tag):
        tu, td = up(4 - k), up(k - 4)
        for i in (0, 1):
            if k > 0 or i == 0:
                value = own(tu, i)
                if k > 1 or (k == 1 and i == 0):
                    recv(pu.at[k - 1, half(i)], (tag, "u", k - 1, i), d_up)
                    value = value + pu[k - 1, half(i), :].astype(F32)
                bu[k, half(i), :] = value.astype(BF)
                send(bu.at[k, half(i)], pu.at[k, half(i)], (tag, "u", k, i), d_up)
            if k > 0 or i == 1:
                value = own(td, i)
                if k > 1 or (k == 1 and i == 1):
                    recv(pd.at[k - 1, half(i)], (tag, "d", k - 1, i), d_dn)
                    value = value + pd[k - 1, half(i), :].astype(F32)
                bd[k, half(i), :] = value.astype(BF)
                send(bd.at[k, half(i)], pd.at[k, half(i)], (tag, "d", k, i), d_dn)

    def rs_final(i, own, pu, pd, tag):
        recv(pu.at[3, half(i)], (tag, "u", 3, i), d_up)
        recv(pd.at[3, half(i)], (tag, "d", 3, i), d_dn)
        return own(z, i) + pu[3, half(i), :].astype(F32) + pd[3, half(i), :].astype(F32)

    uacc[...] = jnp.zeros_like(uacc)
    for j in (1, 2, 3):

        @pl.when(y + j < NY)
        def _(j=j):
            recv(urecv.at[j - 1], ("u", j), d_y[4 - j])
            uacc[...] += urecv[j - 1].astype(F32)

    def own_d(zd, i):
        far = lax.div(z, 4) != lax.div(zd, 4)
        mid = lax.div(z, 2) != lax.div(zd, 2)
        level = jnp.where(far, 2, jnp.where(mid, 1, 0))
        on = (z > zd).astype(F32)
        return uacc[half(i), :] + on * st[level, half(i), :]

    rs_d = functools.partial(rs_step, own=own_d, bu=du, bd=dd, pu=ru, pd=rd, tag="d")
    rs_d(0)

    s34[...] = jnp.zeros_like(s34)
    for j in (1, 2, 3):

        @pl.when(y >= j)
        def _(j=j):
            which = 1 - near if j == 1 else 1
            recv(trecv.at[j - 1], ("t", j), d_y[j])
            s34[which] = s34[which] + trecv[j - 1].astype(F32)

    from_states([s34[0].astype(BF), s34[1].astype(BF)], (5, 6), (None, None))
    for h in range(HH):
        a16 = attf[h].astype(BF)
        att16[:, 128 * h : 128 * h + 128] = a16
        at[y, pl.ds(128 * h, 128), :] = a16.T
    for j in (1, 2, 3):
        send(at.at[y], at.at[y], ("at", j), d_y[j])
    dq_copy = pltpu.make_async_copy(dqv, dq_o, lsem.at[len(loads)])
    dq_copy.start()
    rs_d(1)

    def m_part(index):
        cols = pl.ds(pl.multiple_of(index * 512, 512), 512)
        return mm(att16[...], wo[:, cols]).astype(BF)

    for i in range(NX):
        mp[0, i] = m_part(i * 2 + sib)
    send(mp.at[0], mr, ("m",), d_sib)
    rs_d(2)
    for i in range(NX):
        mp[1, i] = m_part(i * 2 + c)

    for j in (1, 2, 3):
        src = yp(-j)
        recv(bb.at[src, c], ("b", j), d_y[j])
        send(bb.at[src, c], bb.at[src, c], ("b2", j), d_sib)
    recv(mr, ("m",), d_sib)
    for j in (2, 1, 3):
        ms[j - 1] = (mp[1, xp(j)].astype(F32) + mr[xp(j)].astype(F32)).astype(BF)
        send(ms.at[j - 1], mx.at[j - 1], ("mx", j), d_x[j])
    rs_d(3)
    for j in (1, 2, 3):
        recv(bb.at[yp(-j), sib], ("b2", j), d_sib)
    for j in (1, 3, 2):
        recv(at.at[yp(-j)], ("at", j), d_y[j])

    def c_part(n):
        a = jnp.concatenate([at[i] for i in range(NY)], axis=1)
        b = jnp.concatenate(
            [bb[i, n // 2, :, 256 * (n % 2) : 256 * (n % 2) + 256] for i in range(NY)], axis=0
        )
        out = mm(a, b)
        cf[2 * n] = out[:, :128]
        cf[2 * n + 1] = out[:, 128:]

    for n in range(4):
        c_part(n)

    def own_c(zd, i):
        return cf[zd, half(i), :]

    rs_c = functools.partial(rs_step, own=own_c, bu=cu, bd=cd, pu=xu, pd=xd, tag="c")
    rs_c(0)
    rs_c(1)

    for i in (0, 1):
        dn[half(i), :] = rs_final(i, own_d, ru, rd, "d").astype(BF)
    for h in range(HH):
        place = pl.ds(h, 128, stride=HH)
        block = dn[pl.ds(128 * h, 128), :]
        dkv[place, :] = dkv[place, :] + mm(vb[h], block, NT)
        dvv[place, :] = dvv[place, :] + mm(kb[h], block)
    dk_copy = pltpu.make_async_copy(dkv, dk_o, lsem.at[len(loads) + 1])
    dk_copy.start()
    dv_copy = pltpu.make_async_copy(dvv, dv_o, lsem.at[len(loads) + 2])
    dv_copy.start()
    rs_c(2)

    out = mp[1, x].astype(F32) + mr[x].astype(F32)
    for j in (1, 3, 2):
        recv(mx.at[j - 1], ("mx", j), d_x[j])
        out = out + mx[j - 1].astype(F32)
    mixv[...] = out.astype(BF)
    mix_copy = pltpu.make_async_copy(mixv, mixed_o, lsem.at[len(loads) + 3])
    mix_copy.start()
    rs_c(3)
    for i in (0, 1):
        pgv[half(i), :] = rs_final(i, own_c, xu, xd, "c")
    pg_copy = pltpu.make_async_copy(pgv, pg_o, lsem.at[len(loads) + 4])
    pg_copy.start()

    for op in pending:
        op.wait_send()
    for j in (1, 2, 3):

        @pl.when(y >= j)
        def _(j=j):
            which = 1 - near if j == 1 else 1
            rcopy(sty.at[which], urecv.at[j - 1], ids("u", j), d_y[4 - j]).wait_send()

        @pl.when(y + j < NY)
        def _(j=j):
            rcopy(tsend, trecv.at[j - 1], ids("t", j), d_y[j]).wait_send()

    for op in (dq_copy, dk_copy, dv_copy, mix_copy, pg_copy):
        op.wait()
    assert len(ids.table) <= N_SEM, len(ids.table)


N_SEM = 72


def body(queries, keys, values, level_weights, out_proj, out_grad):
    def flat(a):
        return a.reshape(512, 128)

    any_spec = pl.BlockSpec(memory_space=pl.ANY)
    blk = (512, 128)
    v = pltpu.VMEM
    outs = pl.pallas_call(
        body_kernel,
        out_shape=(
            jax.ShapeDtypeStruct((128, 512), BF),
            jax.ShapeDtypeStruct(blk, F32),
            jax.ShapeDtypeStruct(blk, F32),
            jax.ShapeDtypeStruct(blk, F32),
            jax.ShapeDtypeStruct(blk, F32),
        ),
        in_specs=[any_spec] * 6,
        out_specs=[any_spec] * 5,
        scratch_shapes=[
            v(blk, F32), v(blk, F32), v(blk, F32),
            v((7, 4, 128), F32), v((32, 128), F32), v((128, 32), F32),
            v((512, 4096), BF), v((8, 128, 512), BF), v((128, 512), F32),
            v((4, 128, 128), BF), v((4, 128, 128), BF), v((4, 128, 128), BF), v((4, 128, 128), BF),
            v((4, 128, 128), BF), v((4, 128, 128), BF), v((4, 128, 128), F32), v((128, 512), BF),
            v((8, 512, 128), BF), v((3, 512, 128), F32), v((2, 512, 128), BF),
            v(blk, BF), v((3, 512, 128), BF), v((2, 512, 128), F32), v((3, 512, 128), BF), v(blk, F32),
            v((4, 512, 128), BF), v((4, 512, 128), BF), v((4, 512, 128), BF), v((4, 512, 128), BF), v(blk, BF),
            v((4, 2, 128, 512), BF), v((4, 512, 128), BF), v((8, 512, 128), F32),
            v((4, 512, 128), BF), v((4, 512, 128), BF), v((4, 512, 128), BF), v((4, 512, 128), BF),
            v((2, 4, 128, 512), BF), v((4, 128, 512), BF), v((3, 128, 512), BF), v((3, 128, 512), BF),
            v(blk, F32), v(blk, F32), v(blk, F32), v(blk, F32), v((128, 512), BF),
            pltpu.SemaphoreType.DMA((12,)),
            pltpu.SemaphoreType.DMA((N_SEM,)),
            pltpu.SemaphoreType.DMA((N_SEM,)),
        ],
        compiler_params=pltpu.CompilerParams(
            collective_id=0, has_side_effects=True, vmem_limit_bytes=56 << 20
        ),
        name="log_linear",
    )(flat(queries), flat(keys), flat(values), level_weights, out_proj, out_grad)
    mixed, dq, dk, dv, pg = outs
    heads = queries.shape
    return mixed, dq.reshape(heads), dk.reshape(heads), dv.reshape(heads), pg


def solution(mesh):
    placed = (
        P("seq", "head", None),
        P("seq", "head", None),
        P("seq", "head", None),
        P(None, "head", "seq"),
        P("head", None),
        P("seq", "head"),
    )
    return jax.shard_map(
        body,
        mesh=mesh,
        in_specs=placed,
        out_specs=(
            P("seq", "head"),
            P("seq", "head", None),
            P("seq", "head", None),
            P("seq", "head", None),
            P("head", "seq"),
        ),
        check_vma=False,
    )
```

```python
import functools

import jax
import jax.numpy as jnp
from jax import lax
from jax.experimental import pallas as pl
from jax.experimental.pallas import tpu as pltpu
from jax.sharding import PartitionSpec as P

MESH = pl.DeviceIdType.MESH
BF = jnp.bfloat16
F32 = jnp.float32
NN = (((1,), (0,)), ((), ()))
NT = (((1,), (1,)), ((), ()))
TN = (((0,), (0,)), ((), ()))
NY, NZ, NX = 4, 8, 4
HH = 4
HALF = 256


def mm(a, b, dims=NN):
    return lax.dot_general(a, b, dims, preferred_element_type=F32)


class Ids:
    def __init__(self):
        self.table = {}

    def __call__(self, *key):
        return self.table.setdefault(key, len(self.table))


def body_kernel(
    q_h, k_h, v_h, lam_h, wo_h, og_h,
    mixed_o, dq_o, dk_o, dv_o, pg_o,
    qf, kf, vf, lam_v, lam_s, lam_t, wo, gf, gacc,
    qb, kb, vb, gb, pb, db, attf, att16,
    sb, st, sty, tsend, trecv, s34, urecv, uacc,
    du, dd, ru, rd, dn,
    bb, at, cf, cu, cd, xu, xd,
    mp, mr, ms, mx,
    lsem, ssem, rsem,
):
    seq = lax.axis_index("seq")
    hd = lax.axis_index("head")
    y, z = lax.div(seq, NZ), lax.rem(seq, NZ)
    x, c = lax.div(hd, 2), lax.rem(hd, 2)
    sib = 1 - c

    def dev(yy, zz, xx, cc):
        return (yy * NZ + zz, xx * 2 + cc)

    def up(j):
        return lax.rem(z + j + NZ, NZ)

    def yp(j):
        return lax.rem(y + j + NY, NY)

    def xp(j):
        return lax.rem(x + j + NX, NX)

    d_sib = dev(y, z, x, sib)
    d_x = {j: dev(y, z, xp(j), c) for j in (1, 2, 3)}
    d_y = {j: dev(yp(j), z, x, c) for j in (1, 2, 3)}
    d_up, d_dn = dev(y, up(1), x, c), dev(y, up(-1), x, c)

    ids = Ids()
    pending = []

    def rcopy(src, dst, i, device):
        return pltpu.make_async_remote_copy(
            src_ref=src, dst_ref=dst, send_sem=ssem.at[i], recv_sem=rsem.at[i],
            device_id=device, device_id_type=MESH,
        )

    def send(src, dst, key, device):
        op = rcopy(src, dst, ids(*key), device)
        op.start()
        pending.append(op)

    def recv(dst, key, device):
        rcopy(dst, dst, ids(*key), device).wait_recv()

    loads = {}

    def load(name, src, dst):
        op = pltpu.make_async_copy(src, dst, lsem.at[len(loads)])
        op.start()
        loads[name] = op

    load("k", k_h, kf)
    load("v", v_h, vf)
    load("og", og_h, gf.at[hd])
    load("q", q_h, qf)
    load("lam", lam_h, lam_v)
    load("wo", wo_h, wo)

    barrier = pltpu.get_barrier_semaphore()
    partners = [d_sib] + [d_x[j] for j in (1, 2, 3)] + [d_y[j] for j in (1, 2, 3)] + [d_up, d_dn]
    for who in partners:
        pl.semaphore_signal(barrier, inc=1, device_id=who, device_id_type=MESH)

    def head(h):
        return pl.ds(128 * h, 128)

    def rows(ref, h):
        return ref[pl.ds(h, 128, stride=HH), :]

    loads["k"].wait()
    loads["v"].wait()
    for h in range(HH):
        kh = rows(kf, h).astype(BF)
        vh = rows(vf, h).astype(BF)
        kb[h] = kh
        vb[h] = vh
        sb[z, head(h), :] = mm(kh, vh, TN).astype(BF)

    pl.semaphore_wait(barrier, len(partners))

    for j in (1, 3, 2):
        send(og_h, gf.at[hd], ("og", j), d_x[j])

    def ag_send(k, h):
        su, sd = up(-k), up(k)
        if k < 3 or h < 2:
            send(sb.at[su, head(h)], sb.at[su, head(h)], ("agu", k, h), d_up)
        if k < 3 or h >= 2:
            send(sb.at[sd, head(h)], sb.at[sd, head(h)], ("agd", k, h), d_dn)

    def ag_recv(k, h):
        if k < 3 or h < 2:
            recv(sb.at[up(-k - 1), head(h)], ("agu", k, h), d_up)
        if k < 3 or h >= 2:
            recv(sb.at[up(k + 1), head(h)], ("agd", k, h), d_dn)

    def ag_relay(k, heads=range(HH)):
        for h in heads:
            ag_recv(k - 1, h)
            ag_send(k, h)

    for h in range(HH):
        ag_send(0, h)
    send(og_h, gf.at[hd], ("og", 0), d_sib)

    loads["q"].wait()
    loads["lam"].wait()
    lam_s[...] = jnp.zeros_like(lam_s)
    for l in range(7):
        lam_s[pl.ds(4 * l, 4), :] = lam_v[l]
    lam_t[...] = lam_s[...].T

    def lam(l, h):
        return lam_t[:, 4 * l + h : 4 * l + h + 1]

    t_pos = lax.broadcasted_iota(jnp.int32, (128, 128), 0)
    s_pos = lax.broadcasted_iota(jnp.int32, (128, 128), 1)
    causal = t_pos >= s_pos
    cross = (t_pos >= 64) & (s_pos < 64)

    def weight(h):
        return jnp.where(causal, jnp.where(cross, lam(1, h), lam(0, h)), 0.0)

    for h in range(HH):
        qh = rows(qf, h).astype(BF)
        qb[h] = qh
        probs = (mm(qh, kb[h], NT) * weight(h)).astype(BF)
        pb[h] = probs
        attf[h] = mm(probs, vb[h])

    ag_relay(1)

    loads["og"].wait()
    loads["wo"].wait()

    def g_part(index):
        cols = pl.ds(pl.multiple_of(index * 512, 512), 512)
        return mm(gf[index], wo[:, cols], NT)

    gacc[...] = g_part(hd)
    recv(gf.at[x * 2 + sib], ("og", 0), d_sib)
    gacc[...] += g_part(x * 2 + sib)
    ag_relay(2, (0, 1))
    for j in (1, 3, 2):
        src = xp(-j) * 2 + c
        recv(gf.at[src], ("og", j), d_x[j])
        send(gf.at[src], gf.at[src], ("og2", j), d_sib)
    for j in (1, 2, 3):
        send(gf.at[yp(j) * 2 + c], bb.at[y, c], ("b", j), d_y[j])
    ag_relay(2, (2, 3))
    for j in (1, 3, 2):
        gacc[...] += g_part(xp(-j) * 2 + c)
    for j in (1, 3, 2):
        src = xp(-j) * 2 + sib
        recv(gf.at[src], ("og2", j), d_sib)
        gacc[...] += g_part(src)
    for h in range(HH):
        gb[h] = gacc[:, 128 * h : 128 * h + 128].astype(BF)

    def weighted(h, level):
        return (qb[h].astype(F32) * lam(level, h)).astype(BF)

    for d in (4, 3):
        for h in range(HH):
            sty[d - 3, head(h), :] = mm(weighted(h, 2 + d), gb[h], TN).astype(BF)
    near = lax.rem(y, 2)
    for j in (1, 2, 3):

        @pl.when(y >= j)
        def _(j=j):
            which = 1 - near if j == 1 else 1
            rcopy(sty.at[which], urecv.at[j - 1], ids("u", j), d_y[4 - j]).start()

    ag_relay(3)
    for i in (0, 1):
        bb[y, i] = gf[y * 2 + i]
    for d in (0, 1, 2):
        for h in range(HH):
            st[d, head(h), :] = mm(weighted(h, 2 + d), gb[h], TN)

    for i in (0, 1):
        for h in (2 * i, 2 * i + 1):
            ag_recv(3, h)
            total = sb[0, head(h), :].astype(F32)
            for n in range(1, NZ):
                total = total + sb[n, head(h), :].astype(F32)
            tsend[head(h), :] = total.astype(BF)
        part = pl.ds(HALF * i, HALF)
        for j in (1, 2, 3):

            @pl.when(y + j < NY)
            def _(j=j):
                rcopy(tsend.at[part], trecv.at[j - 1, part], ids("t", j, i), d_y[j]).start()

    def local_grads():
        for h in range(HH):
            db[h] = (mm(gb[h], vb[h], NT) * weight(h)).astype(BF)
            dq_o[pl.ds(h, 128, stride=HH), :] = mm(db[h], kb[h])
            dk_o[pl.ds(h, 128, stride=HH), :] = mm(db[h], qb[h], TN)
            dv_o[pl.ds(h, 128, stride=HH), :] = mm(pb[h], gb[h], TN)

    local_grads()

    z1 = z + 1 - 2 * lax.rem(z, 2)
    zp = lax.div(z, 2)
    zp1 = 2 * (zp + 1 - 2 * lax.rem(zp, 2))
    zq1 = 4 * (1 - lax.div(z, 4))
    b0 = lax.rem(z, 2).astype(F32)
    b1 = lax.rem(zp, 2).astype(F32)
    b2 = lax.div(z, 4).astype(F32)

    def from_states(h, states, levels, bits):
        block = jnp.concatenate(states, axis=0)
        wide = jnp.concatenate(states, axis=1)
        qw, gw = [], []
        for l, bit in zip(levels, bits):
            scale = lam(l, h) if bit is None else lam(l, h) * bit
            qw.append((qb[h].astype(F32) * scale).astype(BF))
            gw.append((gb[h].astype(F32) * scale).astype(BF))
        attf[h] += mm(jnp.concatenate(qw, axis=1), block)
        place = pl.ds(h, 128, stride=HH)
        dq_o[place, :] = dq_o[place, :] + mm(jnp.concatenate(gw, axis=1), wide, NT)

    for h in range(HH):
        pair = (sb[zp1, head(h), :].astype(F32) + sb[zp1 + 1, head(h), :].astype(F32)).astype(BF)
        quad = sb[zq1, head(h), :].astype(F32)
        for i in range(1, 4):
            quad = quad + sb[zq1 + i, head(h), :].astype(F32)
        from_states(h, [sb[z1, head(h), :], pair, quad.astype(BF)], (2, 3, 4), (b0, b1, b2))

    class Scatter:
        def __init__(self, tag, own, bu, bd, pu, pd):
            self.tag, self.own = tag, own
            self.side = {"u": (bu, pu, d_up), "d": (bd, pd, d_dn)}

        def step(self, k, h, way):
            first = (h < 2) == (way == "u")
            assert k > 0 or first
            buf, got, device = self.side[way]
            value = self.own(up(4 - k) if way == "u" else up(k - 4), h)
            if k > 1 or (k == 1 and first):
                recv(got.at[k - 1, head(h)], (self.tag, way, k - 1, h), device)
                value = value + got[k - 1, head(h), :].astype(F32)
            buf[k, head(h), :] = value.astype(BF)
            send(buf.at[k, head(h)], got.at[k, head(h)], (self.tag, way, k, h), device)

        def start(self, i):
            for h in (2 * i, 2 * i + 1):
                self.step(0, h, "ud"[i])
            for h in (2 * i, 2 * i + 1):
                self.step(1, h, "du"[i])

        def wave(self, k, pairs=((2, 0), (3, 1), (0, 2), (1, 3))):
            for a, b in pairs:
                self.step(k, a, "u")
                self.step(k, b, "d")

        def wave1(self):
            self.step(1, 0, "u")
            self.step(1, 2, "d")
            self.step(1, 1, "u")
            self.step(1, 3, "d")

        def final(self, h):
            total = self.own(z, h)
            for way in ("u", "d"):
                _, got, device = self.side[way]
                recv(got.at[3, head(h)], (self.tag, way, 3, h), device)
                total = total + got[3, head(h), :].astype(F32)
            return total

    for j in (1, 3, 2):
        src = yp(-j)
        recv(bb.at[src, c], ("b", j), d_y[j])
        send(bb.at[src, c], bb.at[src, c], ("b2", j), d_sib)

    uacc[...] = jnp.zeros_like(uacc)
    for j in (1, 2, 3):

        @pl.when(y + j < NY)
        def _(j=j):
            recv(urecv.at[j - 1], ("u", j), d_y[4 - j])
            uacc[...] += urecv[j - 1].astype(F32)

    def own_d(zd, h):
        far = lax.div(z, 4) != lax.div(zd, 4)
        mid = lax.div(z, 2) != lax.div(zd, 2)
        level = jnp.where(far, 2, jnp.where(mid, 1, 0))
        on = (z > zd).astype(F32)
        return uacc[head(h), :] + on * st[level, head(h), :]

    rs_d = Scatter("d", own_d, du, dd, ru, rd)
    rs_d.start(0)
    rs_d.start(1)

    s34[...] = jnp.zeros_like(s34)
    for i in (0, 1):
        part = pl.ds(HALF * i, HALF)
        for j in (1, 2, 3):

            @pl.when(y >= j)
            def _(j=j):
                which = 1 - near if j == 1 else 1
                recv(trecv.at[j - 1, part], ("t", j, i), d_y[j])
                s34[which, part, :] = s34[which, part, :] + trecv[j - 1, part, :].astype(F32)

        for h in (2 * i, 2 * i + 1):
            from_states(
                h, [s34[0, head(h), :].astype(BF), s34[1, head(h), :].astype(BF)], (5, 6), (None, None)
            )
            a16 = attf[h].astype(BF)
            att16[:, 128 * h : 128 * h + 128] = a16
            at[y, head(h), :] = a16.T
        for j in (1, 3, 2):
            send(at.at[y, part], at.at[y, part], ("at", j, i), d_y[j])
        if i == 0:
            rs_d.wave1()

    def m_part(index):
        cols = pl.ds(pl.multiple_of(index * 512, 512), 512)
        return mm(att16[...], wo[:, cols]).astype(BF)

    for i in range(NX):
        mp[0, i] = m_part(i * 2 + sib)
    send(mp.at[0], mr, ("m",), d_sib)
    rs_d.wave(2)
    for i in range(NX):
        mp[1, i] = m_part(i * 2 + c)
    recv(mr, ("m",), d_sib)
    for j in (1, 3, 2):
        ms[j - 1] = (mp[1, xp(j)].astype(F32) + mr[xp(j)].astype(F32)).astype(BF)
        send(ms.at[j - 1], mx.at[j - 1], ("mx", j), d_x[j])

    for j in (1, 2, 3):
        recv(bb.at[yp(-j), sib], ("b2", j), d_sib)

    def own_c(zd, h):
        return cf[zd, head(h), :]

    rs_c = Scatter("c", own_c, cu, cd, xu, xd)
    for i in (0, 1):
        part = pl.ds(HALF * i, HALF)
        for j in (1, 3, 2):
            recv(at.at[yp(-j), part], ("at", j, i), d_y[j])
        a = jnp.concatenate([at[n, part, :] for n in range(NY)], axis=1)
        for n in range(4):
            b = jnp.concatenate(
                [bb[m, n // 2, :, 256 * (n % 2) : 256 * (n % 2) + 256] for m in range(NY)], axis=0
            )
            out = mm(a, b)
            cf[2 * n, part, :] = out[:, :128]
            cf[2 * n + 1, part, :] = out[:, 128:]
        rs_c.start(i)
    rs_d.wave(3)
    rs_c.wave1()

    for h in range(HH):
        dn[head(h), :] = rs_d.final(h).astype(BF)
    rs_c.wave(2)
    for h in range(HH):
        place = pl.ds(h, 128, stride=HH)
        block = dn[head(h), :]
        dk_o[place, :] = dk_o[place, :] + mm(vb[h], block, NT)
        dv_o[place, :] = dv_o[place, :] + mm(kb[h], block)

    out = mp[1, x].astype(F32) + mr[x].astype(F32)
    for j in (1, 3, 2):
        recv(mx.at[j - 1], ("mx", j), d_x[j])
        out = out + mx[j - 1].astype(F32)
    mixed_o[...] = out.astype(BF)
    rs_c.wave(3)
    for h in (2, 3, 0, 1):
        pg_o[head(h), :] = rs_c.final(h)

    for op in pending:
        op.wait_send()
    for j in (1, 2, 3):

        @pl.when(y >= j)
        def _(j=j):
            which = 1 - near if j == 1 else 1
            rcopy(sty.at[which], urecv.at[j - 1], ids("u", j), d_y[4 - j]).wait_send()

        @pl.when(y + j < NY)
        def _(j=j):
            for i in (0, 1):
                part = pl.ds(HALF * i, HALF)
                rcopy(tsend.at[part], trecv.at[j - 1, part], ids("t", j, i), d_y[j]).wait_send()

    assert len(ids.table) <= N_SEM, len(ids.table)


N_SEM = 120
VLIM = 28


def out_kernel(*refs):
    src, dst, via = refs[:5], refs[5:10], refs[10:15]
    isem, osem = refs[15:]
    ins = [pltpu.make_async_copy(a, b, isem.at[i]) for i, (a, b) in enumerate(zip(src, via))]
    outs = [pltpu.make_async_copy(a, b, osem.at[i]) for i, (a, b) in enumerate(zip(via, dst))]
    for op in ins:
        op.start()
    for a, b in zip(ins, outs):
        a.wait()
        b.start()
    for op in outs:
        op.wait()


def body(queries, keys, values, level_weights, out_proj, out_grad):
    def flat(a):
        return a.reshape(512, 128)

    any_spec = pl.BlockSpec(memory_space=pl.ANY)
    blk = (512, 128)
    v = pltpu.VMEM
    outs = pl.pallas_call(
        body_kernel,
        out_shape=(
            jax.ShapeDtypeStruct((128, 512), BF),
            jax.ShapeDtypeStruct(blk, F32),
            jax.ShapeDtypeStruct(blk, F32),
            jax.ShapeDtypeStruct(blk, F32),
            jax.ShapeDtypeStruct(blk, F32),
        ),
        in_specs=[pl.BlockSpec(memory_space=pltpu.HBM)] * 6,
        out_specs=[pl.BlockSpec(memory_space=pltpu.VMEM)] * 5,
        scratch_shapes=[
            v(blk, F32), v(blk, F32), v(blk, F32),
            v((7, 4, 128), F32), v((32, 128), F32), v((128, 32), F32),
            v((512, 4096), BF), v((8, 128, 512), BF), v((128, 512), F32),
            v((4, 128, 128), BF), v((4, 128, 128), BF), v((4, 128, 128), BF), v((4, 128, 128), BF),
            v((4, 128, 128), BF), v((4, 128, 128), BF), v((4, 128, 128), F32), v((128, 512), BF),
            v((8, 512, 128), BF), v((3, 512, 128), F32), v((2, 512, 128), BF),
            v(blk, BF), v((3, 512, 128), BF), v((2, 512, 128), F32), v((3, 512, 128), BF), v(blk, F32),
            v((4, 512, 128), BF), v((4, 512, 128), BF), v((4, 512, 128), BF), v((4, 512, 128), BF), v(blk, BF),
            v((4, 2, 128, 512), BF), v((4, 512, 128), BF), v((8, 512, 128), F32),
            v((4, 512, 128), BF), v((4, 512, 128), BF), v((4, 512, 128), BF), v((4, 512, 128), BF),
            v((2, 4, 128, 512), BF), v((4, 128, 512), BF), v((3, 128, 512), BF), v((3, 128, 512), BF),
            pltpu.SemaphoreType.DMA((12,)),
            pltpu.SemaphoreType.DMA((N_SEM,)),
            pltpu.SemaphoreType.DMA((N_SEM,)),
        ],
        compiler_params=pltpu.CompilerParams(
            collective_id=0, has_side_effects=True, vmem_limit_bytes=VLIM << 20
        ),
        name="log_linear",
    )(*[pltpu.with_memory_space_constraint(a, pltpu.HBM) for a in (flat(queries), flat(keys), flat(values), level_weights, out_proj, out_grad)])
    mixed, dq, dk, dv, pg = pl.pallas_call(
        out_kernel,
        out_shape=tuple(jax.ShapeDtypeStruct(o.shape, o.dtype) for o in outs),
        in_specs=[any_spec] * 5,
        out_specs=[any_spec] * 5,
        scratch_shapes=[v(o.shape, o.dtype) for o in outs]
        + [pltpu.SemaphoreType.DMA((5,)), pltpu.SemaphoreType.DMA((5,))],
        compiler_params=pltpu.CompilerParams(vmem_limit_bytes=4 << 20),
        name="results",
    )(*outs)
    heads = queries.shape
    return mixed, dq.reshape(heads), dk.reshape(heads), dv.reshape(heads), pg


def solution(mesh):
    placed = (
        P("seq", "head", None),
        P("seq", "head", None),
        P("seq", "head", None),
        P(None, "head", "seq"),
        P("head", None),
        P("seq", "head"),
    )
    return jax.shard_map(
        body,
        mesh=mesh,
        in_specs=placed,
        out_specs=(
            P("seq", "head"),
            P("seq", "head", None),
            P("seq", "head", None),
            P("seq", "head", None),
            P("head", "seq"),
        ),
        check_vma=False,
    )
```

```python
import functools
import math

import jax
import jax.numpy as jnp
from jax import lax
from jax.experimental import pallas as pl
from jax.experimental.pallas import tpu as pltpu
from jax.sharding import PartitionSpec as P

MESH = pl.DeviceIdType.MESH
BF = jnp.bfloat16
F32 = jnp.float32
NN = (((1,), (0,)), ((), ()))
NT = (((1,), (1,)), ((), ()))
TN = (((0,), (0,)), ((), ()))
NY, NZ, NX = 4, 8, 4
HH = 4
HALF = 256


def mm(a, b, dims=NN):
    return lax.dot_general(a, b, dims, preferred_element_type=F32)


class Ids:
    def __init__(self):
        self.table = {}

    def __call__(self, *key):
        return self.table.setdefault(key, len(self.table))


def body_kernel(
    q_h, k_h, v_h, lam_h, wo_h, og_h,
    mixed_o, dq_o, dk_o, dv_o, pg_o,
    qf, kf, vf, lam_v, lam_s, lam_t, wo, gf, gacc,
    qb, kb, vb, gb, pb, db, attf, att16,
    sb, st, sty, tsend, trecv, s34, uwr, us, ur, usum, uall,
    du, dd, ru, rd, dn,
    bb, at, cf, cu, cd, xu, xd,
    mp, mr, ms, mx,
    lsem, ssem, rsem,
):
    seq = lax.axis_index("seq")
    hd = lax.axis_index("head")
    y, z = lax.div(seq, NZ), lax.rem(seq, NZ)
    x, c = lax.div(hd, 2), lax.rem(hd, 2)
    sib = 1 - c

    def dev(yy, zz, xx, cc):
        return (yy * NZ + zz, xx * 2 + cc)

    def up(j):
        return lax.rem(z + j + NZ, NZ)

    def yp(j):
        return lax.rem(y + j + NY, NY)

    def xp(j):
        return lax.rem(x + j + NX, NX)

    d_sib = dev(y, z, x, sib)
    d_x = {j: dev(y, z, xp(j), c) for j in (1, 2, 3)}
    d_y = {j: dev(yp(j), z, x, c) for j in (1, 2, 3)}
    d_up, d_dn = dev(y, up(1), x, c), dev(y, up(-1), x, c)

    ids, sids = Ids(), Ids()
    group = {}

    def rcopy(src, dst, key, device):
        return pltpu.make_async_remote_copy(
            src_ref=src, dst_ref=dst, send_sem=ssem.at[sids(key[0])], recv_sem=rsem.at[ids(*key)],
            device_id=device, device_id_type=MESH,
        )

    def send(src, dst, key, device):
        rcopy(src, dst, key, device).start()
        group[key[0]] = group.get(key[0], 0) + math.prod(src.shape)

    def sent(ref, name):
        pltpu.make_async_remote_copy(
            src_ref=ref, dst_ref=ref, send_sem=ssem.at[sids(name)], recv_sem=rsem.at[0],
            device_id=d_sib, device_id_type=MESH,
        ).wait_send()

    def recv(dst, key, device):
        rcopy(dst, dst, key, device).wait_recv()

    loads = {}

    def load(name, src, dst):
        op = pltpu.make_async_copy(src, dst, lsem.at[len(loads)])
        op.start()
        loads[name] = op

    load("k", k_h, kf)
    load("v", v_h, vf)
    load("og", og_h, gf.at[hd])
    load("q", q_h, qf)
    load("lam", lam_h, lam_v)
    load("wo", wo_h, wo)

    barrier = pltpu.get_barrier_semaphore()
    partners = [d_sib] + [d_x[j] for j in (1, 2, 3)] + [d_y[j] for j in (1, 2, 3)] + [d_up, d_dn]
    for who in partners:
        pl.semaphore_signal(barrier, inc=1, device_id=who, device_id_type=MESH)

    def head(h):
        return pl.ds(128 * h, 128)

    def rows(ref, h):
        return ref[pl.ds(h, 128, stride=HH), :]

    loads["k"].wait()
    loads["v"].wait()
    for h in range(HH):
        kh = rows(kf, h).astype(BF)
        vh = rows(vf, h).astype(BF)
        kb[h] = kh
        vb[h] = vh
        sb[z, head(h), :] = mm(kh, vh, TN).astype(BF)

    pl.semaphore_wait(barrier, len(partners))

    for j in (1, 3, 2):
        send(og_h, gf.at[hd], ("og", j), d_x[j])

    def ag_send(k, h):
        su, sd = up(-k), up(k)
        if k < 3 or h < 2:
            send(sb.at[su, head(h)], sb.at[su, head(h)], ("ag", "u", k, h), d_up)
        if k < 3 or h >= 2:
            send(sb.at[sd, head(h)], sb.at[sd, head(h)], ("ag", "d", k, h), d_dn)

    def ag_recv(k, h):
        if k < 3 or h < 2:
            recv(sb.at[up(-k - 1), head(h)], ("ag", "u", k, h), d_up)
        if k < 3 or h >= 2:
            recv(sb.at[up(k + 1), head(h)], ("ag", "d", k, h), d_dn)

    def ag_relay(k, heads=range(HH)):
        for h in heads:
            ag_recv(k - 1, h)
            ag_send(k, h)

    for h in range(HH):
        ag_send(0, h)
    send(og_h, gf.at[hd], ("og", 0), d_sib)

    loads["q"].wait()
    loads["lam"].wait()
    lam_s[...] = jnp.zeros_like(lam_s)
    for l in range(7):
        lam_s[pl.ds(4 * l, 4), :] = lam_v[l]
    lam_t[...] = lam_s[...].T

    def lam(l, h):
        return lam_t[:, 4 * l + h : 4 * l + h + 1]

    t_pos = lax.broadcasted_iota(jnp.int32, (128, 128), 0)
    s_pos = lax.broadcasted_iota(jnp.int32, (128, 128), 1)
    causal = t_pos >= s_pos
    cross = (t_pos >= 64) & (s_pos < 64)

    def weight(h):
        return jnp.where(causal, jnp.where(cross, lam(1, h), lam(0, h)), 0.0)

    for h in range(HH):
        qh = rows(qf, h).astype(BF)
        qb[h] = qh
        probs = (mm(qh, kb[h], NT) * weight(h)).astype(BF)
        pb[h] = probs
        attf[h] = mm(probs, vb[h])

    ag_relay(1)

    loads["og"].wait()
    loads["wo"].wait()

    def g_part(index):
        cols = pl.ds(pl.multiple_of(index * 512, 512), 512)
        return mm(gf[index], wo[:, cols], NT)

    def og_relay(j):
        src = xp(-j) * 2 + c
        recv(gf.at[src], ("og", j), d_x[j])
        send(gf.at[src], gf.at[src], ("og2", j), d_sib)

    gacc[...] = g_part(hd)
    recv(gf.at[x * 2 + sib], ("og", 0), d_sib)
    gacc[...] += g_part(x * 2 + sib)
    og_relay(1)
    og_relay(3)
    ag_relay(2, (0, 1))
    og_relay(2)
    for j in (1, 2, 3):
        send(gf.at[yp(j) * 2 + c], bb.at[j, c], ("b", j), d_y[j])
    for j in (1, 3, 2):
        gacc[...] += g_part(xp(-j) * 2 + c)
    ag_relay(2, (2, 3))
    for j in (1, 3, 2):
        src = xp(-j) * 2 + sib
        recv(gf.at[src], ("og2", j), d_sib)
        gacc[...] += g_part(src)
    for h in range(HH):
        gb[h] = gacc[:, 128 * h : 128 * h + 128].astype(BF)

    def weighted(h, level):
        return (qb[h].astype(F32) * lam(level, h)).astype(BF)

    for d in (4, 3):
        for h in range(HH):
            sty[d - 3, head(h), :] = mm(weighted(h, 2 + d), gb[h], TN).astype(BF)
    near = lax.rem(y, 2)
    main = jnp.where(y == 1, 0, 1)

    def piece(n):
        return pl.ds(pl.multiple_of(64 * n, 64), 64)

    def u_sum(level, tag):
        for j in range(1, NZ):
            to = up(j)
            rcopy(sty.at[level, piece(to)], uwr.at[level, j - 1], (tag,), dev(y, to, x, c)).start()

    def u_total(level, tag):
        recv(uwr.at[level], (tag,), d_up)
        total = sty[level, piece(z), :].astype(F32)
        for j in range(1, NZ):
            total = total + uwr[level, j - 1].astype(F32)
        us[level] = total.astype(BF)

    ag_relay(3)

    for d in (0, 1, 2):
        for h in range(HH):
            st[d, head(h), :] = mm(weighted(h, 2 + d), gb[h], TN)

    class Scatter:
        def __init__(self, tag, own, bu, bd, pu, pd):
            self.tag, self.own = tag, own
            self.side = {"u": (bu, pu, d_up), "d": (bd, pd, d_dn)}

        def step(self, k, h, way):
            first = (h < 2) == (way == "u")
            assert k > 0 or first
            buf, got, device = self.side[way]
            value = self.own(up(4 - k) if way == "u" else up(k - 4), h)
            if k > 1 or (k == 1 and first):
                recv(got.at[k - 1, head(h)], (self.tag, way, k - 1, h), device)
                value = value + got[k - 1, head(h), :].astype(F32)
            buf[k, head(h), :] = value.astype(BF)
            send(buf.at[k, head(h)], got.at[k, head(h)], (self.tag, way, k, h), device)

        def start(self, i):
            for h in (2 * i, 2 * i + 1):
                self.step(0, h, "ud"[i])
            for h in (2 * i, 2 * i + 1):
                self.step(1, h, "du"[i])

        def wave(self, k, pairs=((2, 0), (3, 1), (0, 2), (1, 3))):
            for a, b in pairs:
                self.step(k, a, "u")
                self.step(k, b, "d")

        def wave1(self):
            self.step(1, 0, "u")
            self.step(1, 2, "d")
            self.step(1, 1, "u")
            self.step(1, 3, "d")

        def final(self, h):
            total = self.own(z, h)
            for way in ("u", "d"):
                _, got, device = self.side[way]
                recv(got.at[3, head(h)], (self.tag, way, 3, h), device)
                total = total + got[3, head(h), :].astype(F32)
            return total

    def own_d(zd, h):
        far = lax.div(z, 4) != lax.div(zd, 4)
        mid = lax.div(z, 2) != lax.div(zd, 2)
        level = jnp.where(far, 2, jnp.where(mid, 1, 0))
        on = (z > zd).astype(F32)
        return on * st[level, head(h), :]

    rs_d = Scatter("d", own_d, du, dd, ru, rd)
    rs_d.start(0)
    rs_d.start(1)
    for i in (0, 1):
        bb[0, i] = gf[y * 2 + i]

    for h in range(HH):
        ag_recv(3, h)
        total = sb[0, head(h), :].astype(F32)
        for n in range(1, NZ):
            total = total + sb[n, head(h), :].astype(F32)
        tsend[head(h), :] = total.astype(BF)
        for j in (1, 2, 3):

            @pl.when(y + j < NY)
            def _(j=j):
                rcopy(tsend.at[head(h)], trecv.at[j - 1, head(h)], ("t%d" % j, h), d_y[j]).start()

    @pl.when(y > 0)
    def _():
        u_sum(main, "u1")

    @pl.when(y == 3)
    def _():
        u_sum(0, "u2")

    for h in range(HH):
        db[h] = (mm(gb[h], vb[h], NT) * weight(h)).astype(BF)
        dq_o[pl.ds(h, 128, stride=HH), :] = mm(db[h], kb[h])
        dk_o[pl.ds(h, 128, stride=HH), :] = mm(db[h], qb[h], TN)
        dv_o[pl.ds(h, 128, stride=HH), :] = mm(pb[h], gb[h], TN)

    z1 = z + 1 - 2 * lax.rem(z, 2)
    zp = lax.div(z, 2)
    zp1 = 2 * (zp + 1 - 2 * lax.rem(zp, 2))
    zq1 = 4 * (1 - lax.div(z, 4))
    b0 = lax.rem(z, 2).astype(F32)
    b1 = lax.rem(zp, 2).astype(F32)
    b2 = lax.div(z, 4).astype(F32)

    def from_states(h, states, levels, bits):
        block = jnp.concatenate(states, axis=0)
        wide = jnp.concatenate(states, axis=1)
        qw, gw = [], []
        for l, bit in zip(levels, bits):
            scale = lam(l, h) if bit is None else lam(l, h) * bit
            qw.append((qb[h].astype(F32) * scale).astype(BF))
            gw.append((gb[h].astype(F32) * scale).astype(BF))
        attf[h] += mm(jnp.concatenate(qw, axis=1), block)
        place = pl.ds(h, 128, stride=HH)
        dq_o[place, :] = dq_o[place, :] + mm(jnp.concatenate(gw, axis=1), wide, NT)

    for h in range(HH):
        pair = (sb[zp1, head(h), :].astype(F32) + sb[zp1 + 1, head(h), :].astype(F32)).astype(BF)
        quad = sb[zq1, head(h), :].astype(F32)
        for i in range(1, 4):
            quad = quad + sb[zq1 + i, head(h), :].astype(F32)
        from_states(h, [sb[z1, head(h), :], pair, quad.astype(BF)], (2, 3, 4), (b0, b1, b2))

    rs_d.wave1()

    for j in (1, 3, 2):
        recv(bb.at[j, c], ("b", j), d_y[j])
        send(bb.at[j, c], bb.at[j, c], ("b2",), d_sib)

    s34[...] = jnp.zeros_like(s34)
    for h in range(HH):
        for j in (1, 2, 3):

            @pl.when(y >= j)
            def _(j=j):
                which = 1 - near if j == 1 else 1
                recv(trecv.at[j - 1, head(h)], ("t%d" % j, h), d_y[j])
                s34[which, head(h), :] = s34[which, head(h), :] + trecv[j - 1, head(h), :].astype(F32)

        from_states(
            h, [s34[0, head(h), :].astype(BF), s34[1, head(h), :].astype(BF)], (5, 6), (None, None)
        )
        a16 = attf[h].astype(BF)
        att16[:, 128 * h : 128 * h + 128] = a16
        at[0, head(h), :] = a16.T
        for j in (1, 3, 2):
            send(at.at[0, head(h)], at.at[j, head(h)], ("at", h), d_y[j])
        if h == 1:
            rs_d.wave(2, ((2, 0), (3, 1)))

    @pl.when(y > 0)
    def _():
        u_total(main, "u1")

    @pl.when(y == 3)
    def _():
        u_total(0, "u2")

    for j in (1, 2, 3):

        @pl.when(y >= j)
        def _(j=j):
            which = 1 - near if j == 1 else 1
            rcopy(us.at[which], ur.at[j - 1], ("u%dy" % j,), d_y[4 - j]).start()

    def m_part(index):
        cols = pl.ds(pl.multiple_of(index * 512, 512), 512)
        return mm(att16[...], wo[:, cols]).astype(BF)

    for i in range(NX):
        mp[0, i] = m_part(i * 2 + sib)
    send(mp.at[0], mr, ("m",), d_sib)
    rs_d.wave(2, ((0, 2), (1, 3)))
    for i in range(NX):
        mp[1, i] = m_part(i * 2 + c)

    recv(bb.at[pl.ds(1, 3), sib], ("b2",), d_sib)

    def later_y():
        @pl.when(y < 3)
        def _():
            usum[...] = jnp.zeros_like(usum)
            for j in (1, 2, 3):

                @pl.when(y + j < NY)
                def _(j=j):
                    recv(ur.at[j - 1], ("u%dy" % j,), d_y[4 - j])
                    usum[...] += ur[j - 1].astype(F32)

            uall[NZ - 1] = usum[...].astype(BF)
            for j in range(1, NZ):
                rcopy(uall.at[NZ - 1], uall.at[j - 1], ("ua",), dev(y, up(j), x, c)).start()

    def own_c(zd, h):
        return cf[zd, head(h), :]

    rs_c = Scatter("c", own_c, cu, cd, xu, xd)
    for i in (0, 1):
        part = pl.ds(HALF * i, HALF)
        for h in (2 * i, 2 * i + 1):
            recv(at.at[pl.ds(1, 3), head(h)], ("at", h), d_y[1])
        a = jnp.concatenate([at[n, part, :] for n in range(NY)], axis=1)
        for n in range(4):
            b = jnp.concatenate(
                [bb[m, n // 2, :, 256 * (n % 2) : 256 * (n % 2) + 256] for m in range(NY)], axis=0
            )
            out = mm(a, b)
            cf[2 * n, part, :] = out[:, :128]
            cf[2 * n + 1, part, :] = out[:, 128:]
        rs_c.start(i)
        if i == 0:
            rs_d.wave(3, ((2, 0), (3, 1)))
            later_y()
    recv(mr, ("m",), d_sib)
    for j in (1, 3, 2):
        ms[j - 1] = (mp[1, xp(j)].astype(F32) + mr[xp(j)].astype(F32)).astype(BF)
        send(ms.at[j - 1], mx.at[j - 1], ("mx",), d_x[j])
    rs_d.wave(3, ((0, 2), (1, 3)))
    rs_c.wave1()

    @pl.when(y < 3)
    def _():
        recv(uall.at[pl.ds(0, NZ - 1)], ("ua",), d_up)

    @pl.when(y == 3)
    def _():
        uall[...] = jnp.zeros_like(uall)

    for h in range(HH):
        own_slots = [lax.rem(z - 2 * h - i + 2 * NZ - 1, NZ) for i in (0, 1)]
        later = jnp.concatenate([uall[n] for n in own_slots], axis=0).astype(F32)
        dn[head(h), :] = (rs_d.final(h) + later).astype(BF)
    rs_c.wave(2)
    for h in range(HH):
        place = pl.ds(h, 128, stride=HH)
        block = dn[head(h), :]
        dk_o[place, :] = dk_o[place, :] + mm(vb[h], block, NT)
        dv_o[place, :] = dv_o[place, :] + mm(kb[h], block)

    out = mp[1, x].astype(F32) + mr[x].astype(F32)
    recv(mx, ("mx",), d_x[1])
    for j in (1, 3, 2):
        out = out + mx[j - 1].astype(F32)
    mixed_o[...] = out.astype(BF)
    rs_c.wave(3)
    for h in (2, 3, 0, 1):
        pg_o[head(h), :] = rs_c.final(h)

    for name, ref in (
        ("og", gf.at[pl.ds(0, 4)]), ("og2", gf.at[pl.ds(0, 3)]), ("b", gf.at[pl.ds(0, 3)]),
        ("b2", gf.at[pl.ds(0, 3)]), ("ag", sb.at[pl.ds(0, 7)]), ("d", sb.at[pl.ds(0, 7)]),
        ("c", sb.at[pl.ds(0, 7)]), ("at", at.at[pl.ds(0, 3)]), ("m", mr), ("mx", mx),
    ):
        assert group[name] == math.prod(ref.shape), (name, group[name])
        sent(ref, name)

    @pl.when(y > 0)
    def _():
        sent(uwr.at[0], "u1")

    @pl.when(y == 3)
    def _():
        sent(uwr.at[0], "u2")

    @pl.when(y < 3)
    def _():
        sent(uwr.at[0], "ua")

    for j in (1, 2, 3):

        @pl.when(y >= j)
        def _(j=j):
            sent(us.at[0], "u%dy" % j)

        @pl.when(y + j < NY)
        def _(j=j):
            sent(tsend, "t%d" % j)

    assert len(sids.table) <= S_SEM and len(ids.table) <= N_SEM, (len(sids.table), len(ids.table))


N_SEM = 119
S_SEM = 19
VLIM = 28


def out_kernel(*refs):
    src, dst, via = refs[:5], refs[5:10], refs[10:15]
    isem, osem = refs[15:]
    ins = [pltpu.make_async_copy(a, b, isem.at[i]) for i, (a, b) in enumerate(zip(src, via))]
    outs = [pltpu.make_async_copy(a, b, osem.at[i]) for i, (a, b) in enumerate(zip(via, dst))]
    for op in ins:
        op.start()
    for a, b in zip(ins, outs):
        a.wait()
        b.start()
    for op in outs:
        op.wait()


def body(queries, keys, values, level_weights, out_proj, out_grad):
    def flat(a):
        return a.reshape(512, 128)

    any_spec = pl.BlockSpec(memory_space=pl.ANY)
    blk = (512, 128)
    v = pltpu.VMEM
    outs = pl.pallas_call(
        body_kernel,
        out_shape=(
            jax.ShapeDtypeStruct((128, 512), BF),
            jax.ShapeDtypeStruct(blk, F32),
            jax.ShapeDtypeStruct(blk, F32),
            jax.ShapeDtypeStruct(blk, F32),
            jax.ShapeDtypeStruct(blk, F32),
        ),
        in_specs=[pl.BlockSpec(memory_space=pltpu.HBM)] * 6,
        out_specs=[pl.BlockSpec(memory_space=pltpu.VMEM)] * 5,
        scratch_shapes=[
            v(blk, F32), v(blk, F32), v(blk, F32),
            v((7, 4, 128), F32), v((32, 128), F32), v((128, 32), F32),
            v((512, 4096), BF), v((8, 128, 512), BF), v((128, 512), F32),
            v((4, 128, 128), BF), v((4, 128, 128), BF), v((4, 128, 128), BF), v((4, 128, 128), BF),
            v((4, 128, 128), BF), v((4, 128, 128), BF), v((4, 128, 128), F32), v((128, 512), BF),
            v((8, 512, 128), BF), v((3, 512, 128), F32), v((2, 512, 128), BF),
            v(blk, BF), v((3, 512, 128), BF), v((2, 512, 128), F32),
            v((2, 7, 64, 128), BF), v((2, 64, 128), BF), v((3, 64, 128), BF), v((64, 128), F32), v((8, 64, 128), BF),
            v((4, 512, 128), BF), v((4, 512, 128), BF), v((4, 512, 128), BF), v((4, 512, 128), BF), v(blk, BF),
            v((4, 2, 128, 512), BF), v((4, 512, 128), BF), v((8, 512, 128), F32),
            v((4, 512, 128), BF), v((4, 512, 128), BF), v((4, 512, 128), BF), v((4, 512, 128), BF),
            v((2, 4, 128, 512), BF), v((4, 128, 512), BF), v((3, 128, 512), BF), v((3, 128, 512), BF),
            pltpu.SemaphoreType.DMA((6,)),
            pltpu.SemaphoreType.DMA((S_SEM,)),
            pltpu.SemaphoreType.DMA((N_SEM,)),
        ],
        compiler_params=pltpu.CompilerParams(
            collective_id=0, has_side_effects=True, vmem_limit_bytes=VLIM << 20
        ),
        name="log_linear",
    )(*[pltpu.with_memory_space_constraint(a, pltpu.HBM) for a in (flat(queries), flat(keys), flat(values), level_weights, out_proj, out_grad)])
    mixed, dq, dk, dv, pg = pl.pallas_call(
        out_kernel,
        out_shape=tuple(jax.ShapeDtypeStruct(o.shape, o.dtype) for o in outs),
        in_specs=[any_spec] * 5,
        out_specs=[any_spec] * 5,
        scratch_shapes=[v(o.shape, o.dtype) for o in outs]
        + [pltpu.SemaphoreType.DMA((5,)), pltpu.SemaphoreType.DMA((5,))],
        compiler_params=pltpu.CompilerParams(vmem_limit_bytes=4 << 20),
        name="results",
    )(*outs)
    heads = queries.shape
    return mixed, dq.reshape(heads), dk.reshape(heads), dv.reshape(heads), pg


def solution(mesh):
    placed = (
        P("seq", "head", None),
        P("seq", "head", None),
        P("seq", "head", None),
        P(None, "head", "seq"),
        P("head", None),
        P("seq", "head"),
    )
    return jax.shard_map(
        body,
        mesh=mesh,
        in_specs=placed,
        out_specs=(
            P("seq", "head"),
            P("seq", "head", None),
            P("seq", "head", None),
            P("seq", "head", None),
            P("head", "seq"),
        ),
        check_vma=False,
    )
```

```python
import functools
import math

import jax
import jax.numpy as jnp
from jax import lax
from jax.experimental import pallas as pl
from jax.experimental.pallas import tpu as pltpu
from jax.sharding import PartitionSpec as P

MESH = pl.DeviceIdType.MESH
BF = jnp.bfloat16
F32 = jnp.float32
NN = (((1,), (0,)), ((), ()))
NT = (((1,), (1,)), ((), ()))
TN = (((0,), (0,)), ((), ()))
NY, NZ, NX = 4, 8, 4
HH = 4
HALF = 256


def mm(a, b, dims=NN):
    return lax.dot_general(a, b, dims, preferred_element_type=F32)


class Ids:
    def __init__(self):
        self.table = {}

    def __call__(self, *key):
        return self.table.setdefault(key, len(self.table))


def body_kernel(
    q_h, k_h, v_h, lam_h, wo_h, og_h,
    mixed_o, dq_o, dk_o, dv_o, pg_o,
    qf, kf, vf, lam_v, lam_s, lam_t, wo, gf, gacc,
    qb, kb, vb, gb, pb, db, attf, att16,
    sb, st, sty, tsend, trecv, tsum, uwr, uwl, us, us2, ur, usum, uo, uall,
    dch, dnear, dsum, dfin,
    bb, at, cf, cu, cd, xu, xd,
    mp, mr, ms, mx,
    lsem, ssem, rsem,
):
    seq = lax.axis_index("seq")
    hd = lax.axis_index("head")
    y, z = lax.div(seq, NZ), lax.rem(seq, NZ)
    x, c = lax.div(hd, 2), lax.rem(hd, 2)
    sib = 1 - c

    def dev(yy, zz, xx, cc):
        return (yy * NZ + zz, xx * 2 + cc)

    def up(j):
        return lax.rem(z + j + NZ, NZ)

    def yp(j):
        return lax.rem(y + j + NY, NY)

    def xp(j):
        return lax.rem(x + j + NX, NX)

    d_sib = dev(y, z, x, sib)
    d_x = {j: dev(y, z, xp(j), c) for j in (1, 2, 3)}
    d_y = {j: dev(yp(j), z, x, c) for j in (1, 2, 3)}
    d_up, d_dn = dev(y, up(1), x, c), dev(y, up(-1), x, c)

    ids, sids = Ids(), Ids()
    group = {}

    def rcopy(src, dst, key, device):
        return pltpu.make_async_remote_copy(
            src_ref=src, dst_ref=dst, send_sem=ssem.at[sids(key[0])], recv_sem=rsem.at[ids(*key)],
            device_id=device, device_id_type=MESH,
        )

    def send(src, dst, key, device):
        rcopy(src, dst, key, device).start()
        group[key[0]] = group.get(key[0], 0) + math.prod(src.shape)

    def sent(ref, name):
        pltpu.make_async_remote_copy(
            src_ref=ref, dst_ref=ref, send_sem=ssem.at[sids(name)], recv_sem=rsem.at[0],
            device_id=d_sib, device_id_type=MESH,
        ).wait_send()

    def recv(dst, key, device):
        rcopy(dst, dst, key, device).wait_recv()

    loads = {}

    def load(name, src, dst):
        op = pltpu.make_async_copy(src, dst, lsem.at[len(loads)])
        op.start()
        loads[name] = op

    load("k", k_h, kf)
    load("v", v_h, vf)
    load("og", og_h, gf.at[hd])
    load("q", q_h, qf)
    load("lam", lam_h, lam_v)
    load("wo", wo_h, wo)

    barrier = pltpu.get_barrier_semaphore()
    partners = [d_sib] + [d_x[j] for j in (1, 2, 3)] + [d_y[j] for j in (1, 2, 3)] + [d_up, d_dn]
    for who in partners:
        pl.semaphore_signal(barrier, inc=1, device_id=who, device_id_type=MESH)

    def head(h):
        return pl.ds(128 * h, 128)

    def rows(ref, h):
        return ref[pl.ds(h, 128, stride=HH), :]

    loads["k"].wait()
    loads["v"].wait()
    for h in range(HH):
        kh = rows(kf, h).astype(BF)
        vh = rows(vf, h).astype(BF)
        kb[h] = kh
        vb[h] = vh
        sb[z, head(h), :] = mm(kh, vh, TN).astype(BF)

    pl.semaphore_wait(barrier, len(partners))

    for j in (1, 3, 2):
        send(og_h, gf.at[hd], ("og", j), d_x[j])

    def ag_send(k, h):
        su, sd = up(-k), up(k)
        if k < 3 or h < 2:
            send(sb.at[su, head(h)], sb.at[su, head(h)], ("ag", "u", k, h), d_up)
        if k < 3 or h >= 2:
            send(sb.at[sd, head(h)], sb.at[sd, head(h)], ("ag", "d", k, h), d_dn)

    def ag_recv(k, h):
        if k < 3 or h < 2:
            recv(sb.at[up(-k - 1), head(h)], ("ag", "u", k, h), d_up)
        if k < 3 or h >= 2:
            recv(sb.at[up(k + 1), head(h)], ("ag", "d", k, h), d_dn)

    def ag_relay(k, heads=range(HH)):
        for h in heads:
            ag_recv(k - 1, h)
            ag_send(k, h)

    for h in range(HH):
        ag_send(0, h)
    send(og_h, gf.at[hd], ("og", 0), d_sib)

    loads["q"].wait()
    loads["lam"].wait()
    lam_s[...] = jnp.zeros_like(lam_s)
    for l in range(7):
        lam_s[pl.ds(4 * l, 4), :] = lam_v[l]
    lam_t[...] = lam_s[...].T

    def lam(l, h):
        return lam_t[:, 4 * l + h : 4 * l + h + 1]

    t_pos = lax.broadcasted_iota(jnp.int32, (128, 128), 0)
    s_pos = lax.broadcasted_iota(jnp.int32, (128, 128), 1)
    causal = t_pos >= s_pos
    cross = (t_pos >= 64) & (s_pos < 64)

    def weight(h):
        return jnp.where(causal, jnp.where(cross, lam(1, h), lam(0, h)), 0.0)

    for h in range(HH):
        qh = rows(qf, h).astype(BF)
        qb[h] = qh
        probs = (mm(qh, kb[h], NT) * weight(h)).astype(BF)
        pb[h] = probs
        attf[h] = mm(probs, vb[h])

    ag_relay(1)

    loads["og"].wait()
    loads["wo"].wait()

    def g_part(index):
        cols = pl.ds(pl.multiple_of(index * 512, 512), 512)
        return mm(gf[index], wo[:, cols], NT)

    def og_relay(j):
        src = xp(-j) * 2 + c
        recv(gf.at[src], ("og", j), d_x[j])
        send(gf.at[src], gf.at[src], ("og2", j), d_sib)

    gacc[...] = g_part(hd)
    recv(gf.at[x * 2 + sib], ("og", 0), d_sib)
    gacc[...] += g_part(x * 2 + sib)
    og_relay(1)
    og_relay(3)
    ag_relay(2, (0, 1))
    og_relay(2)
    for j in (1, 2, 3):
        send(gf.at[yp(j) * 2 + c], bb.at[j, c], ("b", j), d_y[j])
    ag_relay(2, (2, 3))
    for j in (1, 3, 2):
        gacc[...] += g_part(xp(-j) * 2 + c)

    def g_far(j):
        src = xp(-j) * 2 + sib
        recv(gf.at[src], ("og2", j), d_sib)
        gacc[...] += g_part(src)

    g_far(1)
    g_far(3)
    ag_relay(3, (0, 1))
    g_far(2)
    for h in range(HH):
        gb[h] = gacc[:, 128 * h : 128 * h + 128].astype(BF)
    ag_relay(3, (2, 3))

    def weighted(h, level):
        return (qb[h].astype(F32) * lam(level, h)).astype(BF)

    for d in (4, 3, 2):
        for h in range(HH):
            sty[{3: 0, 4: 1, 2: 2}[d], head(h), :] = mm(weighted(h, 2 + d), gb[h], TN).astype(BF)
    near = lax.rem(y, 2)
    main = jnp.where(y == 1, 0, 1)

    def piece(n):
        return pl.ds(pl.multiple_of(64 * n, 64), 64)

    def u_sum(level, tag):
        for j in range(1, NZ):
            to = up(j)
            rcopy(sty.at[level, piece(to)], uwr.at[level, j - 1], (tag,), dev(y, to, x, c)).start()

    def u_total(level, tag):
        recv(uwr.at[level], (tag,), d_up)
        total = sty[level, piece(z), :].astype(F32)
        for j in range(1, NZ):
            total = total + uwr[level, j - 1].astype(F32)
        us[level] = total.astype(BF)

    def half_sum():
        for j in range(1, NZ):
            to = up(j)
            rcopy(sty.at[2, piece(to)], uwl.at[z - 4], ("u0",), dev(y, to, x, c)).start()

    def half_total():
        @pl.when(z < 4)
        def _():
            recv(uwl, ("u0",), d_up)

        @pl.when(z >= 4)
        def _():
            uwl[z - 4] = sty[2, piece(z), :]
            recv(uwl.at[pl.ds(0, 3)], ("u0",), d_up)

        us2[...] = sum(uwl[i].astype(F32) for i in range(4))


    for d in (1, 0):
        for h in range(HH):
            st[d, head(h), :] = mm(weighted(h, 2 + d), gb[h], TN).astype(BF)

    place4 = lax.rem(z, 4)

    @pl.when(place4 == 3)
    def _():
        for h in range(HH):
            rcopy(st.at[1, head(h)], dch.at[head(h)], ("d", h), d_dn).start()
        rcopy(st.at[0], dnear, ("d0",), d_dn).start()

    def chain(level):
        for h in range(HH):
            recv(dch.at[head(h)], ("d", h), d_dn)
            total = dch[head(h), :].astype(F32) + st[level, head(h), :].astype(F32)
            dsum[head(h), :] = total.astype(BF)
            rcopy(dsum.at[head(h)], dch.at[head(h)], ("d", h), d_dn).start()

    class Scatter:
        def __init__(self, tag, own, bu, bd, pu, pd):
            self.tag, self.own = tag, own
            self.side = {"u": (bu, pu, d_up), "d": (bd, pd, d_dn)}

        def step(self, k, h, way):
            first = (h < 2) == (way == "u")
            assert k > 0 or first
            buf, got, device = self.side[way]
            value = self.own(up(4 - k) if way == "u" else up(k - 4), h)
            if k > 1 or (k == 1 and first):
                recv(got.at[k - 1, head(h)], (self.tag, way, k - 1, h), device)
                value = value + got[k - 1, head(h), :].astype(F32)
            buf[k, head(h), :] = value.astype(BF)
            send(buf.at[k, head(h)], got.at[k, head(h)], (self.tag, way, k, h), device)

        def start(self, i):
            for h in (2 * i, 2 * i + 1):
                self.step(0, h, "ud"[i])
                self.step(1, h, "du"[i])

        def wave(self, i, k):
            for h in (2 * i, 2 * i + 1):
                self.step(k, h, "ud"[i])
                if k < 3:
                    self.step(k + 1, h, "du"[i])

        def final(self, h):
            total = self.own(z, h)
            for way in ("u", "d"):
                _, got, device = self.side[way]
                recv(got.at[3, head(h)], (self.tag, way, 3, h), device)
                total = total + got[3, head(h), :].astype(F32)
            return total

    for i in (0, 1):
        bb[0, i] = gf[y * 2 + i]

    for h in range(HH):
        ag_recv(3, h)
        total = sb[0, head(h), :].astype(F32)
        for n in range(1, NZ):
            total = total + sb[n, head(h), :].astype(F32)
        tsend[head(h), :] = total.astype(BF)

        @pl.when((y == 0) | (y == 2))
        def _(h=h):
            rcopy(tsend.at[head(h)], trecv.at[0, head(h)], ("t", h), d_y[1]).start()

        @pl.when(y == 1)
        def _(h=h):
            rcopy(tsend.at[head(h)], trecv.at[0, head(h)], ("t", h), d_y[3]).start()

    @pl.when(y > 0)
    def _():
        u_sum(main, "u1")

    @pl.when(y == 3)
    def _():
        u_sum(0, "u2")

    @pl.when(z >= 4)
    def _():
        half_sum()

    for h in range(HH):
        db[h] = (mm(gb[h], vb[h], NT) * weight(h)).astype(BF)
        dq_o[pl.ds(h, 128, stride=HH), :] = mm(db[h], kb[h])
        dk_o[pl.ds(h, 128, stride=HH), :] = mm(db[h], qb[h], TN)
        dv_o[pl.ds(h, 128, stride=HH), :] = mm(pb[h], gb[h], TN)

    @pl.when(y < 2)
    def _():
        for h in range(HH):
            recv(trecv.at[0, head(h)], ("t", h), d_y[1])
            both = tsend[head(h), :].astype(F32) + trecv[0, head(h), :].astype(F32)
            tsum[head(h), :] = both.astype(BF)

            @pl.when(y == 1)
            def _(h=h):
                rcopy(tsum.at[head(h)], trecv.at[1, head(h)], ("tt", h), d_y[1]).start()

            @pl.when(y == 0)
            def _(h=h):
                rcopy(tsum.at[head(h)], trecv.at[1, head(h)], ("tt", h), d_y[3]).start()

    z1 = z + 1 - 2 * lax.rem(z, 2)
    zp = lax.div(z, 2)
    zp1 = 2 * (zp + 1 - 2 * lax.rem(zp, 2))
    zq1 = 4 * (1 - lax.div(z, 4))
    b0 = lax.rem(z, 2).astype(F32)
    b1 = lax.rem(zp, 2).astype(F32)
    b2 = lax.div(z, 4).astype(F32)

    def from_states(h, states, levels, bits):
        block = jnp.concatenate(states, axis=0)
        wide = jnp.concatenate(states, axis=1)
        qw, gw = [], []
        for l, bit in zip(levels, bits):
            scale = lam(l, h) if bit is None else lam(l, h) * bit
            qw.append((qb[h].astype(F32) * scale).astype(BF))
            gw.append((gb[h].astype(F32) * scale).astype(BF))
        attf[h] += mm(jnp.concatenate(qw, axis=1), block)
        place = pl.ds(h, 128, stride=HH)
        dq_o[place, :] = dq_o[place, :] + mm(jnp.concatenate(gw, axis=1), wide, NT)

    for h in range(HH):
        pair = (sb[zp1, head(h), :].astype(F32) + sb[zp1 + 1, head(h), :].astype(F32)).astype(BF)
        quad = sb[zq1, head(h), :].astype(F32)
        for i in range(1, 4):
            quad = quad + sb[zq1 + i, head(h), :].astype(F32)
        from_states(h, [sb[z1, head(h), :], pair, quad.astype(BF)], (2, 3, 4), (b0, b1, b2))

    for j in (1, 3, 2):
        recv(bb.at[j, c], ("b", j), d_y[j])
        send(bb.at[j, c], bb.at[j, c], ("b2",), d_sib)

    @pl.when(place4 == 2)
    def _():
        chain(1)

    @pl.when(y == 0)
    def _():
        trecv[...] = jnp.zeros_like(trecv)

    @pl.when(y == 1)
    def _():
        trecv[1] = jnp.zeros_like(tsend)

    @pl.when(y == 2)
    def _():
        trecv[0] = jnp.zeros_like(tsend)

    for h in range(HH):

        @pl.when(y == 3)
        def _(h=h):
            recv(trecv.at[0, head(h)], ("t", h), d_y[1])

        @pl.when(y >= 2)
        def _(h=h):
            recv(trecv.at[1, head(h)], ("tt", h), d_y[1])

        from_states(h, [trecv[0, head(h), :], trecv[1, head(h), :]], (5, 6), (None, None))
        a16 = attf[h].astype(BF)
        att16[:, 128 * h : 128 * h + 128] = a16
        at[0, head(h), :] = a16.T
        for j in (1, 3, 2):
            send(at.at[0, head(h)], at.at[j, head(h)], ("at", h), d_y[j])

    @pl.when(place4 == 1)
    def _():
        chain(0)

    def m_part(index):
        cols = pl.ds(pl.multiple_of(index * 512, 512), 512)
        return mm(att16[...], wo[:, cols]).astype(BF)

    for i in range(NX):
        mp[0, i] = m_part(i * 2 + sib)
    send(mp.at[0], mr, ("m",), d_sib)
    for i in range(NX):
        mp[1, i] = m_part(i * 2 + c)

    def own_c(zd, h):
        return cf[zd, head(h), :]

    rs_c = Scatter("c", own_c, cu, cd, xu, xd)

    def product(i):
        part = pl.ds(HALF * i, HALF)
        for h in (2 * i, 2 * i + 1):
            recv(at.at[pl.ds(1, 3), head(h)], ("at", h), d_y[1])
        a = jnp.concatenate([at[n, part, :] for n in range(NY)], axis=1)
        for n in range(4):
            b = jnp.concatenate(
                [bb[m, n // 2, :, 256 * (n % 2) : 256 * (n % 2) + 256] for m in range(NY)], axis=0
            )
            out = mm(a, b)
            cf[2 * n, part, :] = out[:, :128]
            cf[2 * n + 1, part, :] = out[:, 128:]
        rs_c.start(i)

    recv(bb.at[pl.ds(1, 3), sib], ("b2",), d_sib)
    product(0)

    def u_send(j, level):
        rcopy(us.at[level], ur.at[j - 1], ("u%dy" % j,), d_y[4 - j]).start()

    @pl.when(y > 0)
    def _():
        u_total(main, "u1")

    @pl.when(y == 1)
    def _():
        u_send(1, 0)

    @pl.when(y == 2)
    def _():
        u_send(1, 1)
        u_send(2, 1)

    @pl.when(y == 3)
    def _():
        u_send(2, 1)
        u_send(3, 1)

    product(1)
    recv(mr, ("m",), d_sib)
    for j in (1, 3, 2):
        ms[j - 1] = (mp[1, xp(j)].astype(F32) + mr[xp(j)].astype(F32)).astype(BF)
        send(ms.at[j - 1], mx.at[j - 1], ("mx",), d_x[j])
    rs_c.wave(0, 1)

    @pl.when(y == 3)
    def _():
        u_total(0, "u2")
        u_send(1, 0)

    half_total()

    rs_c.wave(1, 1)

    def later_all():
        usum[...] = jnp.zeros_like(usum)
        for j in (1, 2, 3):

            @pl.when(y + j < NY)
            def _(j=j):
                recv(ur.at[j - 1], ("u%dy" % j,), d_y[4 - j])
                usum[...] += ur[j - 1].astype(F32)

        uo[0] = usum[...].astype(BF)
        uo[1] = (usum[...] + us2[...]).astype(BF)
        uall[NZ - 1] = uo[jnp.where(z < 4, 1, 0)]
        for j in range(1, NZ):
            to = up(j)

            @pl.when((y < 3) | (to < 4))
            def _(j=j, to=to):
                low = jnp.where(to < 4, 1, 0)
                rcopy(uo.at[low], uall.at[j - 1], ("ua",), dev(y, to, x, c)).start()

    later_all()
    rs_c.wave(0, 2)
    rs_c.wave(1, 2)
    rs_c.wave(0, 3)
    rs_c.wave(1, 3)

    out = mp[1, x].astype(F32) + mr[x].astype(F32)
    recv(mx, ("mx",), d_x[1])
    for j in (1, 3, 2):
        out = out + mx[j - 1].astype(F32)
    mixed_o[...] = out.astype(BF)

    some = (y < 3) | (z < 4)

    @pl.when(some)
    def _():
        recv(uall.at[pl.ds(0, NZ - 1)], ("ua",), d_up)

    @pl.when(jnp.logical_not(some))
    def _():
        uall[...] = jnp.zeros_like(uall)

    @pl.when(place4 == 0)
    def _():
        for h in range(HH):
            recv(dch.at[head(h)], ("d", h), d_dn)
        dfin[...] = dch[...]

    @pl.when(place4 == 1)
    def _():
        dfin[...] = dch[...]

    @pl.when(place4 == 2)
    def _():
        recv(dnear, ("d0",), d_dn)
        dfin[...] = dnear[...]

    @pl.when(place4 == 3)
    def _():
        dfin[...] = jnp.zeros_like(dfin)

    for h in range(HH):
        own_slots = [lax.rem(z - 2 * h - i + 2 * NZ - 1, NZ) for i in (0, 1)]
        later = jnp.concatenate([uall[n] for n in own_slots], axis=0).astype(F32)
        block = (dfin[head(h), :].astype(F32) + later).astype(BF)
        place = pl.ds(h, 128, stride=HH)
        dk_o[place, :] = dk_o[place, :] + mm(vb[h], block, NT)
        dv_o[place, :] = dv_o[place, :] + mm(kb[h], block)

    for h in (0, 1, 2, 3):
        pg_o[head(h), :] = rs_c.final(h)

    for name, ref in (
        ("og", gf.at[pl.ds(0, 4)]), ("og2", gf.at[pl.ds(0, 3)]), ("b", gf.at[pl.ds(0, 3)]),
        ("b2", gf.at[pl.ds(0, 3)]), ("ag", sb.at[pl.ds(0, 7)]),
        ("c", sb.at[pl.ds(0, 7)]), ("at", at.at[pl.ds(0, 3)]), ("m", mr), ("mx", mx),
    ):
        assert group[name] == math.prod(ref.shape), (name, group[name])
        sent(ref, name)

    @pl.when(y > 0)
    def _():
        sent(uwr.at[0], "u1")

    @pl.when(y == 3)
    def _():
        sent(uwr.at[0], "u2")

    @pl.when(y < 3)
    def _():
        sent(uwr.at[0], "ua")

    @pl.when((y == 3) & (z < 4))
    def _():
        sent(uwl.at[pl.ds(0, 3)], "ua")

    @pl.when((y == 3) & (z >= 4))
    def _():
        sent(uwl, "ua")

    @pl.when(z >= 4)
    def _():
        sent(uwr.at[0], "u0")

    @pl.when(place4 > 0)
    def _():
        sent(dch, "d")

    @pl.when(place4 == 3)
    def _():
        sent(dnear, "d0")

    @pl.when(y < 3)
    def _():
        sent(tsend, "t")

    @pl.when(y < 2)
    def _():
        sent(tsend, "tt")

    for j in (1, 2, 3):

        @pl.when(y >= j)
        def _(j=j):
            sent(us.at[0], "u%dy" % j)

    assert len(sids.table) <= S_SEM and len(ids.table) <= N_SEM, (len(sids.table), len(ids.table))


N_SEM = 97
S_SEM = 21
VLIM = 28


def out_kernel(*refs):
    src, dst, via = refs[:5], refs[5:10], refs[10:15]
    isem, osem = refs[15:]
    ins = [pltpu.make_async_copy(a, b, isem.at[i]) for i, (a, b) in enumerate(zip(src, via))]
    outs = [pltpu.make_async_copy(a, b, osem.at[i]) for i, (a, b) in enumerate(zip(via, dst))]
    for op in ins:
        op.start()
    for a, b in zip(ins, outs):
        a.wait()
        b.start()
    for op in outs:
        op.wait()


def body(queries, keys, values, level_weights, out_proj, out_grad):
    def flat(a):
        return a.reshape(512, 128)

    any_spec = pl.BlockSpec(memory_space=pl.ANY)
    blk = (512, 128)
    v = pltpu.VMEM
    outs = pl.pallas_call(
        body_kernel,
        out_shape=(
            jax.ShapeDtypeStruct((128, 512), BF),
            jax.ShapeDtypeStruct(blk, F32),
            jax.ShapeDtypeStruct(blk, F32),
            jax.ShapeDtypeStruct(blk, F32),
            jax.ShapeDtypeStruct(blk, F32),
        ),
        in_specs=[pl.BlockSpec(memory_space=pltpu.HBM)] * 6,
        out_specs=[pl.BlockSpec(memory_space=pltpu.VMEM)] * 5,
        scratch_shapes=[
            v(blk, F32), v(blk, F32), v(blk, F32),
            v((7, 4, 128), F32), v((32, 128), F32), v((128, 32), F32),
            v((512, 4096), BF), v((8, 128, 512), BF), v((128, 512), F32),
            v((4, 128, 128), BF), v((4, 128, 128), BF), v((4, 128, 128), BF), v((4, 128, 128), BF),
            v((4, 128, 128), BF), v((4, 128, 128), BF), v((4, 128, 128), F32), v((128, 512), BF),
            v((8, 512, 128), BF), v((2, 512, 128), BF), v((3, 512, 128), BF),
            v(blk, BF), v((2, 512, 128), BF), v(blk, BF),
            v((2, 7, 64, 128), BF), v((4, 64, 128), BF), v((2, 64, 128), BF), v((64, 128), F32), v((3, 64, 128), BF),
            v((64, 128), F32), v((2, 64, 128), BF), v((8, 64, 128), BF),
            v(blk, BF), v(blk, BF), v(blk, BF), v(blk, BF),
            v((4, 2, 128, 512), BF), v((4, 512, 128), BF), v((8, 512, 128), F32),
            v((4, 512, 128), BF), v((4, 512, 128), BF), v((4, 512, 128), BF), v((4, 512, 128), BF),
            v((2, 4, 128, 512), BF), v((4, 128, 512), BF), v((3, 128, 512), BF), v((3, 128, 512), BF),
            pltpu.SemaphoreType.DMA((6,)),
            pltpu.SemaphoreType.DMA((S_SEM,)),
            pltpu.SemaphoreType.DMA((N_SEM,)),
        ],
        compiler_params=pltpu.CompilerParams(
            collective_id=0, has_side_effects=True, vmem_limit_bytes=VLIM << 20
        ),
        name="log_linear",
    )(*[pltpu.with_memory_space_constraint(a, pltpu.HBM) for a in (flat(queries), flat(keys), flat(values), level_weights, out_proj, out_grad)])
    mixed, dq, dk, dv, pg = pl.pallas_call(
        out_kernel,
        out_shape=tuple(jax.ShapeDtypeStruct(o.shape, o.dtype) for o in outs),
        in_specs=[any_spec] * 5,
        out_specs=[any_spec] * 5,
        scratch_shapes=[v(o.shape, o.dtype) for o in outs]
        + [pltpu.SemaphoreType.DMA((5,)), pltpu.SemaphoreType.DMA((5,))],
        compiler_params=pltpu.CompilerParams(vmem_limit_bytes=4 << 20),
        name="results",
    )(*outs)
    heads = queries.shape
    return mixed, dq.reshape(heads), dk.reshape(heads), dv.reshape(heads), pg


def solution(mesh):
    placed = (
        P("seq", "head", None),
        P("seq", "head", None),
        P("seq", "head", None),
        P(None, "head", "seq"),
        P("head", None),
        P("seq", "head"),
    )
    return jax.shard_map(
        body,
        mesh=mesh,
        in_specs=placed,
        out_specs=(
            P("seq", "head"),
            P("seq", "head", None),
            P("seq", "head", None),
            P("seq", "head", None),
            P("head", "seq"),
        ),
        check_vma=False,
    )
```

```python
import functools
import math

import jax
import jax.numpy as jnp
from jax import lax
from jax.experimental import pallas as pl
from jax.experimental.pallas import tpu as pltpu
from jax.sharding import PartitionSpec as P

MESH = pl.DeviceIdType.MESH
BF = jnp.bfloat16
F32 = jnp.float32
NN = (((1,), (0,)), ((), ()))
NT = (((1,), (1,)), ((), ()))
TN = (((0,), (0,)), ((), ()))
NY, NZ, NX = 4, 8, 4
HH = 4
HALF = 256


def mm(a, b, dims=NN):
    return lax.dot_general(a, b, dims, preferred_element_type=F32)


class Ids:
    def __init__(self):
        self.table = {}

    def __call__(self, *key):
        return self.table.setdefault(key, len(self.table))


def body_kernel(
    q_h, k_h, v_h, lam_h, wo_h, og_h,
    mixed_o, dq_o, dk_o, dv_o, pg_o,
    qf, kf, vf, lam_v, lam_s, lam_t, wo, gf, gacc,
    qb, kb, vb, gb, pb, db, attf, att16,
    sb, st, sty, tsend, trecv, tsum, uwr, uwl, us, us2, ur, usum, uo, uall,
    dch, dnear, dsum, dfin,
    bb, at, cf, cu, cd, xu, xd,
    mp, mr, ms, mx,
    lsem, ssem, rsem,
):
    seq = lax.axis_index("seq")
    hd = lax.axis_index("head")
    y, z = lax.div(seq, NZ), lax.rem(seq, NZ)
    x, c = lax.div(hd, 2), lax.rem(hd, 2)
    sib = 1 - c

    def dev(yy, zz, xx, cc):
        return (yy * NZ + zz, xx * 2 + cc)

    def up(j):
        return lax.rem(z + j + NZ, NZ)

    def yp(j):
        return lax.rem(y + j + NY, NY)

    def xp(j):
        return lax.rem(x + j + NX, NX)

    d_sib = dev(y, z, x, sib)
    d_x = {j: dev(y, z, xp(j), c) for j in (1, 2, 3)}
    d_y = {j: dev(yp(j), z, x, c) for j in (1, 2, 3)}
    d_up, d_dn = dev(y, up(1), x, c), dev(y, up(-1), x, c)

    ids, sids = Ids(), Ids()
    group = {}

    def rcopy(src, dst, key, device):
        return pltpu.make_async_remote_copy(
            src_ref=src, dst_ref=dst, send_sem=ssem.at[sids(key[0])], recv_sem=rsem.at[ids(*key)],
            device_id=device, device_id_type=MESH,
        )

    def send(src, dst, key, device):
        rcopy(src, dst, key, device).start()
        group[key[0]] = group.get(key[0], 0) + math.prod(src.shape)

    def sent(ref, name):
        pltpu.make_async_remote_copy(
            src_ref=ref, dst_ref=ref, send_sem=ssem.at[sids(name)], recv_sem=rsem.at[0],
            device_id=d_sib, device_id_type=MESH,
        ).wait_send()

    def recv(dst, key, device):
        rcopy(dst, dst, key, device).wait_recv()

    loads = {}

    def load(name, src, dst):
        op = pltpu.make_async_copy(src, dst, lsem.at[len(loads)])
        op.start()
        loads[name] = op

    load("k", k_h, kf)
    load("v", v_h, vf)
    load("og", og_h, gf.at[hd])
    load("q", q_h, qf)
    load("lam", lam_h, lam_v)
    load("wo", wo_h, wo)

    barrier = pltpu.get_barrier_semaphore()
    partners = [d_sib] + [d_x[j] for j in (1, 2, 3)] + [d_y[j] for j in (1, 2, 3)] + [d_up, d_dn]
    for who in partners:
        pl.semaphore_signal(barrier, inc=1, device_id=who, device_id_type=MESH)

    def head(h):
        return pl.ds(128 * h, 128)

    def rows(ref, h):
        return ref[pl.ds(h, 128, stride=HH), :]

    loads["k"].wait()
    loads["v"].wait()
    def ag_send(k, h):
        su, sd = up(-k), up(k)
        if k < 3 or h < 2:
            send(sb.at[su, head(h)], sb.at[su, head(h)], ("ag", "u", k, h), d_up)
        if k < 3 or h >= 2:
            send(sb.at[sd, head(h)], sb.at[sd, head(h)], ("ag", "d", k, h), d_dn)

    def ag_recv(k, h):
        if k < 3 or h < 2:
            recv(sb.at[up(-k - 1), head(h)], ("ag", "u", k, h), d_up)
        if k < 3 or h >= 2:
            recv(sb.at[up(k + 1), head(h)], ("ag", "d", k, h), d_dn)

    def ag_relay(k, heads=range(HH)):
        for h in heads:
            ag_recv(k - 1, h)
            ag_send(k, h)

    def key_value_sum(h):
        kh = rows(kf, h).astype(BF)
        vh = rows(vf, h).astype(BF)
        kb[h] = kh
        vb[h] = vh
        sb[z, head(h), :] = mm(kh, vh, TN).astype(BF)

    key_value_sum(0)
    pl.semaphore_wait(barrier, len(partners))
    ag_send(0, 0)
    key_value_sum(1)
    ag_send(0, 1)

    for j in (1, 3, 2):
        send(og_h, gf.at[hd], ("og", j), d_x[j])
    for h in (2, 3):
        key_value_sum(h)
        ag_send(0, h)
    send(og_h, gf.at[hd], ("og", 0), d_sib)

    loads["q"].wait()
    loads["lam"].wait()
    lam_s[...] = jnp.zeros_like(lam_s)
    for l in range(7):
        lam_s[pl.ds(4 * l, 4), :] = lam_v[l]
    lam_t[...] = lam_s[...].T

    def lam(l, h):
        return lam_t[:, 4 * l + h : 4 * l + h + 1]

    t_pos = lax.broadcasted_iota(jnp.int32, (128, 128), 0)
    s_pos = lax.broadcasted_iota(jnp.int32, (128, 128), 1)
    causal = t_pos >= s_pos
    cross = (t_pos >= 64) & (s_pos < 64)

    def weight(h):
        return jnp.where(causal, jnp.where(cross, lam(1, h), lam(0, h)), 0.0)

    for h in range(HH):
        qh = rows(qf, h).astype(BF)
        qb[h] = qh
        probs = (mm(qh, kb[h], NT) * weight(h)).astype(BF)
        pb[h] = probs
        attf[h] = mm(probs, vb[h])

    ag_relay(1)

    loads["og"].wait()
    loads["wo"].wait()

    def g_part(index):
        cols = pl.ds(pl.multiple_of(index * 512, 512), 512)
        return mm(gf[index], wo[:, cols], NT)

    def og_relay(j):
        src = xp(-j) * 2 + c
        recv(gf.at[src], ("og", j), d_x[j])
        send(gf.at[src], gf.at[src], ("og2", j), d_sib)

    gacc[...] = g_part(hd)
    recv(gf.at[x * 2 + sib], ("og", 0), d_sib)
    gacc[...] += g_part(x * 2 + sib)
    og_relay(1)
    og_relay(3)
    ag_relay(2)
    og_relay(2)
    for j in (1, 2, 3):
        send(gf.at[yp(j) * 2 + c], bb.at[j, c], ("b", j), d_y[j])
    for j in (1, 3, 2):
        gacc[...] += g_part(xp(-j) * 2 + c)

    def g_far(j):
        src = xp(-j) * 2 + sib
        recv(gf.at[src], ("og2", j), d_sib)
        gacc[...] += g_part(src)

    g_far(1)
    g_far(3)
    ag_relay(3, (0, 1))
    g_far(2)
    for h in range(HH):
        gb[h] = gacc[:, 128 * h : 128 * h + 128].astype(BF)
    ag_relay(3, (2, 3))

    def weighted(h, level):
        return (qb[h].astype(F32) * lam(level, h)).astype(BF)

    for d in (4, 3, 2):
        for h in range(HH):
            sty[{3: 0, 4: 1, 2: 2}[d], head(h), :] = mm(weighted(h, 2 + d), gb[h], TN).astype(BF)
    near = lax.rem(y, 2)
    main = jnp.where(y == 1, 0, 1)

    def piece(n):
        return pl.ds(pl.multiple_of(64 * n, 64), 64)

    def u_sum(level, tag):
        for j in range(1, NZ):
            to = up(j)
            rcopy(sty.at[level, piece(to)], uwr.at[level, j - 1], (tag,), dev(y, to, x, c)).start()

    def u_total(level, tag):
        recv(uwr.at[level], (tag,), d_up)
        total = sty[level, piece(z), :].astype(F32)
        for j in range(1, NZ):
            total = total + uwr[level, j - 1].astype(F32)
        us[level] = total.astype(BF)

    def half_sum():
        for j in range(1, NZ):
            to = up(j)
            rcopy(sty.at[2, piece(to)], uwl.at[z - 4], ("u0",), dev(y, to, x, c)).start()

    def half_total():
        @pl.when(z < 4)
        def _():
            recv(uwl, ("u0",), d_up)

        @pl.when(z >= 4)
        def _():
            uwl[z - 4] = sty[2, piece(z), :]
            recv(uwl.at[pl.ds(0, 3)], ("u0",), d_up)

        us2[...] = sum(uwl[i].astype(F32) for i in range(4))


    def level_sum(h):
        ag_recv(3, h)
        total = sb[0, head(h), :].astype(F32)
        for n in range(1, NZ):
            total = total + sb[n, head(h), :].astype(F32)
        tsend[head(h), :] = total.astype(BF)

        @pl.when((y == 0) | (y == 2))
        def _():
            rcopy(tsend.at[head(h)], trecv.at[0, head(h)], ("t", h), d_y[1]).start()

        @pl.when(y == 1)
        def _():
            rcopy(tsend.at[head(h)], trecv.at[0, head(h)], ("t", h), d_y[3]).start()

    level_sum(0)
    level_sum(1)

    for d in (1, 0):
        for h in range(HH):
            st[d, head(h), :] = mm(weighted(h, 2 + d), gb[h], TN).astype(BF)

    place4 = lax.rem(z, 4)

    @pl.when(place4 == 3)
    def _():
        for h in range(HH):
            rcopy(st.at[1, head(h)], dch.at[head(h)], ("d", h), d_dn).start()
        rcopy(st.at[0], dnear, ("d0",), d_dn).start()

    def chain(level):
        for h in range(HH):
            recv(dch.at[head(h)], ("d", h), d_dn)
            total = dch[head(h), :].astype(F32) + st[level, head(h), :].astype(F32)
            dsum[head(h), :] = total.astype(BF)
            rcopy(dsum.at[head(h)], dch.at[head(h)], ("d", h), d_dn).start()

    class Scatter:
        def __init__(self, tag, own, bu, bd, pu, pd):
            self.tag, self.own = tag, own
            self.side = {"u": (bu, pu, d_up), "d": (bd, pd, d_dn)}

        def step(self, k, h, way):
            first = (h < 2) == (way == "u")
            assert k > 0 or first
            buf, got, device = self.side[way]
            value = self.own(up(4 - k) if way == "u" else up(k - 4), h)
            if k > 1 or (k == 1 and first):
                recv(got.at[k - 1, head(h)], (self.tag, way, k - 1, h), device)
                value = value + got[k - 1, head(h), :].astype(F32)
            buf[k, head(h), :] = value.astype(BF)
            send(buf.at[k, head(h)], got.at[k, head(h)], (self.tag, way, k, h), device)

        def start(self, i):
            for h in (2 * i, 2 * i + 1):
                self.step(0, h, "ud"[i])
                self.step(1, h, "du"[i])

        def wave(self, i, k):
            for h in (2 * i, 2 * i + 1):
                self.step(k, h, "ud"[i])
                if k < 3:
                    self.step(k + 1, h, "du"[i])

        def final(self, h):
            total = self.own(z, h)
            for way in ("u", "d"):
                _, got, device = self.side[way]
                recv(got.at[3, head(h)], (self.tag, way, 3, h), device)
                total = total + got[3, head(h), :].astype(F32)
            return total

    for i in (0, 1):
        bb[0, i] = gf[y * 2 + i]

    level_sum(2)
    level_sum(3)

    @pl.when(y > 0)
    def _():
        u_sum(main, "u1")

    @pl.when(y == 3)
    def _():
        u_sum(0, "u2")

    @pl.when(z >= 4)
    def _():
        half_sum()

    for h in range(HH):
        db[h] = (mm(gb[h], vb[h], NT) * weight(h)).astype(BF)
        dq_o[pl.ds(h, 128, stride=HH), :] = mm(db[h], kb[h])
        dk_o[pl.ds(h, 128, stride=HH), :] = mm(db[h], qb[h], TN)
        dv_o[pl.ds(h, 128, stride=HH), :] = mm(pb[h], gb[h], TN)

    @pl.when(y < 2)
    def _():
        for h in range(HH):
            recv(trecv.at[0, head(h)], ("t", h), d_y[1])
            both = tsend[head(h), :].astype(F32) + trecv[0, head(h), :].astype(F32)
            tsum[head(h), :] = both.astype(BF)

            @pl.when(y == 1)
            def _(h=h):
                rcopy(tsum.at[head(h)], trecv.at[1, head(h)], ("tt", h), d_y[1]).start()

            @pl.when(y == 0)
            def _(h=h):
                rcopy(tsum.at[head(h)], trecv.at[1, head(h)], ("tt", h), d_y[3]).start()

    z1 = z + 1 - 2 * lax.rem(z, 2)
    zp = lax.div(z, 2)
    zp1 = 2 * (zp + 1 - 2 * lax.rem(zp, 2))
    zq1 = 4 * (1 - lax.div(z, 4))
    b0 = lax.rem(z, 2).astype(F32)
    b1 = lax.rem(zp, 2).astype(F32)
    b2 = lax.div(z, 4).astype(F32)

    def from_states(h, states, levels, bits):
        block = jnp.concatenate(states, axis=0)
        wide = jnp.concatenate(states, axis=1)
        qw, gw = [], []
        for l, bit in zip(levels, bits):
            scale = lam(l, h) if bit is None else lam(l, h) * bit
            qw.append((qb[h].astype(F32) * scale).astype(BF))
            gw.append((gb[h].astype(F32) * scale).astype(BF))
        attf[h] += mm(jnp.concatenate(qw, axis=1), block)
        place = pl.ds(h, 128, stride=HH)
        dq_o[place, :] = dq_o[place, :] + mm(jnp.concatenate(gw, axis=1), wide, NT)

    for h in range(HH):
        pair = (sb[zp1, head(h), :].astype(F32) + sb[zp1 + 1, head(h), :].astype(F32)).astype(BF)
        quad = sb[zq1, head(h), :].astype(F32)
        for i in range(1, 4):
            quad = quad + sb[zq1 + i, head(h), :].astype(F32)
        from_states(h, [sb[z1, head(h), :], pair, quad.astype(BF)], (2, 3, 4), (b0, b1, b2))

    for j in (1, 3, 2):
        recv(bb.at[j, c], ("b", j), d_y[j])
        send(bb.at[j, c], bb.at[j, c], ("b2",), d_sib)

    @pl.when(place4 == 2)
    def _():
        chain(1)

    @pl.when(y == 0)
    def _():
        trecv[...] = jnp.zeros_like(trecv)

    @pl.when(y == 1)
    def _():
        trecv[1] = jnp.zeros_like(tsend)

    @pl.when(y == 2)
    def _():
        trecv[0] = jnp.zeros_like(tsend)

    for h in range(HH):

        @pl.when(y == 3)
        def _(h=h):
            recv(trecv.at[0, head(h)], ("t", h), d_y[1])

        @pl.when(y >= 2)
        def _(h=h):
            recv(trecv.at[1, head(h)], ("tt", h), d_y[1])

        from_states(h, [trecv[0, head(h), :], trecv[1, head(h), :]], (5, 6), (None, None))
        a16 = attf[h].astype(BF)
        att16[:, 128 * h : 128 * h + 128] = a16
        at[0, head(h), :] = a16.T
        for j in (2, 1, 3):
            send(at.at[0, head(h)], at.at[j, head(h)], ("at", h), d_y[j])

    @pl.when(place4 == 1)
    def _():
        chain(0)

    def m_part(index):
        cols = pl.ds(pl.multiple_of(index * 512, 512), 512)
        return mm(att16[...], wo[:, cols]).astype(BF)

    for i in range(NX):
        mp[0, i] = m_part(i * 2 + sib)
    send(mp.at[0], mr, ("m",), d_sib)
    for i in range(NX):
        mp[1, i] = m_part(i * 2 + c)

    def own_c(zd, h):
        return cf[zd, head(h), :]

    rs_c = Scatter("c", own_c, cu, cd, xu, xd)

    def product(i):
        part = pl.ds(HALF * i, HALF)
        for h in (2 * i, 2 * i + 1):
            recv(at.at[pl.ds(1, 3), head(h)], ("at", h), d_y[1])
        a = jnp.concatenate([at[n, part, :] for n in range(NY)], axis=1)
        for n in range(4):
            b = jnp.concatenate(
                [bb[m, n // 2, :, 256 * (n % 2) : 256 * (n % 2) + 256] for m in range(NY)], axis=0
            )
            out = mm(a, b)
            cf[2 * n, part, :] = out[:, :128]
            cf[2 * n + 1, part, :] = out[:, 128:]
        rs_c.start(i)

    recv(bb.at[pl.ds(1, 3), sib], ("b2",), d_sib)
    product(0)

    def u_send(j, level):
        rcopy(us.at[level], ur.at[j - 1], ("u%dy" % j,), d_y[4 - j]).start()

    @pl.when(y > 0)
    def _():
        u_total(main, "u1")

    @pl.when(y == 1)
    def _():
        u_send(1, 0)

    @pl.when(y == 2)
    def _():
        u_send(1, 1)
        u_send(2, 1)

    @pl.when(y == 3)
    def _():
        u_send(2, 1)
        u_send(3, 1)

    product(1)
    rs_c.wave(0, 1)
    recv(mr, ("m",), d_sib)
    for j in (1, 3, 2):
        ms[j - 1] = (mp[1, xp(j)].astype(F32) + mr[xp(j)].astype(F32)).astype(BF)
        send(ms.at[j - 1], mx.at[j - 1], ("mx",), d_x[j])

    @pl.when(y == 3)
    def _():
        u_total(0, "u2")
        u_send(1, 0)

    half_total()

    rs_c.wave(1, 1)

    rs_c.wave(0, 2)

    def later_all():
        usum[...] = jnp.zeros_like(usum)
        for j in (1, 2, 3):

            @pl.when(y + j < NY)
            def _(j=j):
                recv(ur.at[j - 1], ("u%dy" % j,), d_y[4 - j])
                usum[...] += ur[j - 1].astype(F32)

        uo[0] = usum[...].astype(BF)
        uo[1] = (usum[...] + us2[...]).astype(BF)
        uall[NZ - 1] = uo[jnp.where(z < 4, 1, 0)]
        for j in range(1, NZ):
            to = up(j)

            @pl.when((y < 3) | (to < 4))
            def _(j=j, to=to):
                low = jnp.where(to < 4, 1, 0)
                rcopy(uo.at[low], uall.at[j - 1], ("ua",), dev(y, to, x, c)).start()

    later_all()
    rs_c.wave(1, 2)

    rs_c.wave(0, 3)
    rs_c.wave(1, 3)

    out = mp[1, x].astype(F32) + mr[x].astype(F32)
    recv(mx, ("mx",), d_x[1])
    for j in (1, 3, 2):
        out = out + mx[j - 1].astype(F32)
    mixed_o[...] = out.astype(BF)

    some = (y < 3) | (z < 4)

    @pl.when(some)
    def _():
        recv(uall.at[pl.ds(0, NZ - 1)], ("ua",), d_up)

    @pl.when(jnp.logical_not(some))
    def _():
        uall[...] = jnp.zeros_like(uall)

    @pl.when(place4 == 0)
    def _():
        for h in range(HH):
            recv(dch.at[head(h)], ("d", h), d_dn)
        dfin[...] = dch[...]

    @pl.when(place4 == 1)
    def _():
        dfin[...] = dch[...]

    @pl.when(place4 == 2)
    def _():
        recv(dnear, ("d0",), d_dn)
        dfin[...] = dnear[...]

    @pl.when(place4 == 3)
    def _():
        dfin[...] = jnp.zeros_like(dfin)

    for h in range(HH):
        own_slots = [lax.rem(z - 2 * h - i + 2 * NZ - 1, NZ) for i in (0, 1)]
        later = jnp.concatenate([uall[n] for n in own_slots], axis=0).astype(F32)
        block = (dfin[head(h), :].astype(F32) + later).astype(BF)
        place = pl.ds(h, 128, stride=HH)
        dk_o[place, :] = dk_o[place, :] + mm(vb[h], block, NT)
        dv_o[place, :] = dv_o[place, :] + mm(kb[h], block)

    for h in (0, 1, 2, 3):
        pg_o[head(h), :] = rs_c.final(h)

    for name, ref in (
        ("og", gf.at[pl.ds(0, 4)]), ("og2", gf.at[pl.ds(0, 3)]), ("b", gf.at[pl.ds(0, 3)]),
        ("b2", gf.at[pl.ds(0, 3)]), ("ag", sb.at[pl.ds(0, 7)]),
        ("c", sb.at[pl.ds(0, 7)]), ("at", at.at[pl.ds(0, 3)]), ("m", mr), ("mx", mx),
    ):
        assert group[name] == math.prod(ref.shape), (name, group[name])
        sent(ref, name)

    @pl.when(y > 0)
    def _():
        sent(uwr.at[0], "u1")

    @pl.when(y == 3)
    def _():
        sent(uwr.at[0], "u2")

    @pl.when(y < 3)
    def _():
        sent(uwr.at[0], "ua")

    @pl.when((y == 3) & (z < 4))
    def _():
        sent(uwl.at[pl.ds(0, 3)], "ua")

    @pl.when((y == 3) & (z >= 4))
    def _():
        sent(uwl, "ua")

    @pl.when(z >= 4)
    def _():
        sent(uwr.at[0], "u0")

    @pl.when(place4 > 0)
    def _():
        sent(dch, "d")

    @pl.when(place4 == 3)
    def _():
        sent(dnear, "d0")

    @pl.when(y < 3)
    def _():
        sent(tsend, "t")

    @pl.when(y < 2)
    def _():
        sent(tsend, "tt")

    for j in (1, 2, 3):

        @pl.when(y >= j)
        def _(j=j):
            sent(us.at[0], "u%dy" % j)

    assert len(sids.table) <= S_SEM and len(ids.table) <= N_SEM, (len(sids.table), len(ids.table))


N_SEM = 97
S_SEM = 21
VLIM = 28


def out_kernel(*refs):
    src, dst, via = refs[:5], refs[5:10], refs[10:15]
    isem, osem = refs[15:]
    ins = [pltpu.make_async_copy(a, b, isem.at[i]) for i, (a, b) in enumerate(zip(src, via))]
    outs = [pltpu.make_async_copy(a, b, osem.at[i]) for i, (a, b) in enumerate(zip(via, dst))]
    for op in ins:
        op.start()
    for a, b in zip(ins, outs):
        a.wait()
        b.start()
    for op in outs:
        op.wait()


def body(queries, keys, values, level_weights, out_proj, out_grad):
    def flat(a):
        return a.reshape(512, 128)

    any_spec = pl.BlockSpec(memory_space=pl.ANY)
    blk = (512, 128)
    v = pltpu.VMEM
    outs = pl.pallas_call(
        body_kernel,
        out_shape=(
            jax.ShapeDtypeStruct((128, 512), BF),
            jax.ShapeDtypeStruct(blk, F32),
            jax.ShapeDtypeStruct(blk, F32),
            jax.ShapeDtypeStruct(blk, F32),
            jax.ShapeDtypeStruct(blk, F32),
        ),
        in_specs=[pl.BlockSpec(memory_space=pltpu.HBM)] * 6,
        out_specs=[pl.BlockSpec(memory_space=pltpu.VMEM)] * 5,
        scratch_shapes=[
            v(blk, F32), v(blk, F32), v(blk, F32),
            v((7, 4, 128), F32), v((32, 128), F32), v((128, 32), F32),
            v((512, 4096), BF), v((8, 128, 512), BF), v((128, 512), F32),
            v((4, 128, 128), BF), v((4, 128, 128), BF), v((4, 128, 128), BF), v((4, 128, 128), BF),
            v((4, 128, 128), BF), v((4, 128, 128), BF), v((4, 128, 128), F32), v((128, 512), BF),
            v((8, 512, 128), BF), v((2, 512, 128), BF), v((3, 512, 128), BF),
            v(blk, BF), v((2, 512, 128), BF), v(blk, BF),
            v((2, 7, 64, 128), BF), v((4, 64, 128), BF), v((2, 64, 128), BF), v((64, 128), F32), v((3, 64, 128), BF),
            v((64, 128), F32), v((2, 64, 128), BF), v((8, 64, 128), BF),
            v(blk, BF), v(blk, BF), v(blk, BF), v(blk, BF),
            v((4, 2, 128, 512), BF), v((4, 512, 128), BF), v((8, 512, 128), F32),
            v((4, 512, 128), BF), v((4, 512, 128), BF), v((4, 512, 128), BF), v((4, 512, 128), BF),
            v((2, 4, 128, 512), BF), v((4, 128, 512), BF), v((3, 128, 512), BF), v((3, 128, 512), BF),
            pltpu.SemaphoreType.DMA((6,)),
            pltpu.SemaphoreType.DMA((S_SEM,)),
            pltpu.SemaphoreType.DMA((N_SEM,)),
        ],
        compiler_params=pltpu.CompilerParams(
            collective_id=0, has_side_effects=True, vmem_limit_bytes=VLIM << 20
        ),
        name="log_linear",
    )(*[pltpu.with_memory_space_constraint(a, pltpu.HBM) for a in (flat(queries), flat(keys), flat(values), level_weights, out_proj, out_grad)])
    mixed, dq, dk, dv, pg = pl.pallas_call(
        out_kernel,
        out_shape=tuple(jax.ShapeDtypeStruct(o.shape, o.dtype) for o in outs),
        in_specs=[any_spec] * 5,
        out_specs=[any_spec] * 5,
        scratch_shapes=[v(o.shape, o.dtype) for o in outs]
        + [pltpu.SemaphoreType.DMA((5,)), pltpu.SemaphoreType.DMA((5,))],
        compiler_params=pltpu.CompilerParams(vmem_limit_bytes=4 << 20),
        name="results",
    )(*outs)
    heads = queries.shape
    return mixed, dq.reshape(heads), dk.reshape(heads), dv.reshape(heads), pg


def solution(mesh):
    placed = (
        P("seq", "head", None),
        P("seq", "head", None),
        P("seq", "head", None),
        P(None, "head", "seq"),
        P("head", None),
        P("seq", "head"),
    )
    return jax.shard_map(
        body,
        mesh=mesh,
        in_specs=placed,
        out_specs=(
            P("seq", "head"),
            P("seq", "head", None),
            P("seq", "head", None),
            P("seq", "head", None),
            P("head", "seq"),
        ),
        check_vma=False,
    )
```

```python
import functools
import math

import jax
import jax.numpy as jnp
from jax import lax
from jax.experimental import pallas as pl
from jax.experimental.pallas import tpu as pltpu
from jax.sharding import PartitionSpec as P

MESH = pl.DeviceIdType.MESH
BF = jnp.bfloat16
F32 = jnp.float32
NN = (((1,), (0,)), ((), ()))
NT = (((1,), (1,)), ((), ()))
TN = (((0,), (0,)), ((), ()))
NY, NZ, NX = 4, 8, 4
HH = 4
HALF = 256


def mm(a, b, dims=NN):
    return lax.dot_general(a, b, dims, preferred_element_type=F32)


class Ids:
    def __init__(self):
        self.table = {}

    def __call__(self, *key):
        return self.table.setdefault(key, len(self.table))


def body_kernel(
    q_h, k_h, v_h, lam_h, wo_h, og_h,
    mixed_o, dq_o, dk_o, dv_o, pg_o,
    qf, kf, vf, lam_v, lam_s, lam_t, wo, gf, gacc,
    qb, kb, vb, gb, pb, db, attf, att16,
    sb, st, sty, tsend, trecv, tsum, uwr, uwl, us, us2, ur, usum, uo, uall,
    dch, dnear, dsum, dfin,
    bb, at, cf, cu, cd, xu, xd,
    mp, mr, ms, mx,
    lsem, ssem, rsem,
):
    seq = lax.axis_index("seq")
    hd = lax.axis_index("head")
    y, z = lax.div(seq, NZ), lax.rem(seq, NZ)
    x, c = lax.div(hd, 2), lax.rem(hd, 2)
    sib = 1 - c

    def dev(yy, zz, xx, cc):
        return (yy * NZ + zz, xx * 2 + cc)

    def up(j):
        return lax.rem(z + j + NZ, NZ)

    def yp(j):
        return lax.rem(y + j + NY, NY)

    def xp(j):
        return lax.rem(x + j + NX, NX)

    d_sib = dev(y, z, x, sib)
    d_x = {j: dev(y, z, xp(j), c) for j in (1, 2, 3)}
    d_y = {j: dev(yp(j), z, x, c) for j in (1, 2, 3)}
    d_up, d_dn = dev(y, up(1), x, c), dev(y, up(-1), x, c)

    ids, sids = Ids(), Ids()
    group = {}

    def rcopy(src, dst, key, device):
        return pltpu.make_async_remote_copy(
            src_ref=src, dst_ref=dst, send_sem=ssem.at[sids(key[0])], recv_sem=rsem.at[ids(*key)],
            device_id=device, device_id_type=MESH,
        )

    def send(src, dst, key, device):
        rcopy(src, dst, key, device).start()
        group[key[0]] = group.get(key[0], 0) + math.prod(src.shape)

    def sent(ref, name):
        pltpu.make_async_remote_copy(
            src_ref=ref, dst_ref=ref, send_sem=ssem.at[sids(name)], recv_sem=rsem.at[0],
            device_id=d_sib, device_id_type=MESH,
        ).wait_send()

    def recv(dst, key, device):
        rcopy(dst, dst, key, device).wait_recv()

    loads = {}

    def load(name, src, dst):
        op = pltpu.make_async_copy(src, dst, lsem.at[len(loads)])
        op.start()
        loads[name] = op

    load("k", k_h, kf)
    load("v", v_h, vf)
    load("og", og_h, gf.at[hd])
    load("q", q_h, qf)
    load("lam", lam_h, lam_v)
    load("wo", wo_h, wo)

    barrier = pltpu.get_barrier_semaphore()
    partners = [d_sib] + [d_x[j] for j in (1, 2, 3)] + [d_y[j] for j in (1, 2, 3)] + [d_up, d_dn]
    for who in partners:
        pl.semaphore_signal(barrier, inc=1, device_id=who, device_id_type=MESH)

    def head(h):
        return pl.ds(128 * h, 128)

    def rows(ref, h):
        return ref[pl.ds(h, 128, stride=HH), :]

    loads["k"].wait()
    loads["v"].wait()
    for h in range(HH):
        kh = rows(kf, h).astype(BF)
        vh = rows(vf, h).astype(BF)
        kb[h] = kh
        vb[h] = vh
        sb[z, head(h), :] = mm(kh, vh, TN).astype(BF)

    pl.semaphore_wait(barrier, len(partners))

    for j in (1, 3, 2):
        send(og_h, gf.at[hd], ("og", j), d_x[j])

    def ag_send(k, h):
        su, sd = up(-k), up(k)
        if k < 3 or h < 2:
            send(sb.at[su, head(h)], sb.at[su, head(h)], ("ag", "u", k, h), d_up)
        if k < 3 or h >= 2:
            send(sb.at[sd, head(h)], sb.at[sd, head(h)], ("ag", "d", k, h), d_dn)

    def ag_recv(k, h):
        if k < 3 or h < 2:
            recv(sb.at[up(-k - 1), head(h)], ("ag", "u", k, h), d_up)
        if k < 3 or h >= 2:
            recv(sb.at[up(k + 1), head(h)], ("ag", "d", k, h), d_dn)

    def ag_relay(k, heads=range(HH)):
        for h in heads:
            ag_recv(k - 1, h)
            ag_send(k, h)

    for h in range(HH):
        ag_send(0, h)
    send(og_h, gf.at[hd], ("og", 0), d_sib)

    loads["q"].wait()
    loads["lam"].wait()
    lam_s[...] = jnp.zeros_like(lam_s)
    for l in range(7):
        lam_s[pl.ds(4 * l, 4), :] = lam_v[l]
    lam_t[...] = lam_s[...].T

    def lam(l, h):
        return lam_t[:, 4 * l + h : 4 * l + h + 1]

    t_pos = lax.broadcasted_iota(jnp.int32, (128, 128), 0)
    s_pos = lax.broadcasted_iota(jnp.int32, (128, 128), 1)
    causal = t_pos >= s_pos
    cross = (t_pos >= 64) & (s_pos < 64)

    def weight(h):
        return jnp.where(causal, jnp.where(cross, lam(1, h), lam(0, h)), 0.0)

    for h in range(HH):
        qh = rows(qf, h).astype(BF)
        qb[h] = qh
        probs = (mm(qh, kb[h], NT) * weight(h)).astype(BF)
        pb[h] = probs
        attf[h] = mm(probs, vb[h])

    ag_relay(1)

    loads["og"].wait()
    loads["wo"].wait()

    def g_part(index):
        cols = pl.ds(pl.multiple_of(index * 512, 512), 512)
        return mm(gf[index], wo[:, cols], NT)

    def og_relay(j):
        src = xp(-j) * 2 + c
        recv(gf.at[src], ("og", j), d_x[j])
        send(gf.at[src], gf.at[src], ("og2", j), d_sib)

    gacc[...] = g_part(hd)
    recv(gf.at[x * 2 + sib], ("og", 0), d_sib)
    gacc[...] += g_part(x * 2 + sib)
    og_relay(1)
    og_relay(3)
    ag_relay(2, (0, 1))
    og_relay(2)
    for j in (1, 2, 3):
        send(gf.at[yp(j) * 2 + c], bb.at[j, c], ("b", j), d_y[j])
    ag_relay(2, (2, 3))
    for j in (1, 3, 2):
        gacc[...] += g_part(xp(-j) * 2 + c)

    def g_far(j):
        src = xp(-j) * 2 + sib
        recv(gf.at[src], ("og2", j), d_sib)
        gacc[...] += g_part(src)

    g_far(1)
    g_far(3)
    ag_relay(3, (0, 1))
    g_far(2)
    for h in range(HH):
        gb[h] = gacc[:, 128 * h : 128 * h + 128].astype(BF)
    ag_relay(3, (2, 3))

    def weighted(h, level):
        return (qb[h].astype(F32) * lam(level, h)).astype(BF)

    for d in (4, 3, 2):
        for h in range(HH):
            sty[{3: 0, 4: 1, 2: 2}[d], head(h), :] = mm(weighted(h, 2 + d), gb[h], TN).astype(BF)
    near = lax.rem(y, 2)
    main = jnp.where(y == 1, 0, 1)

    def piece(n):
        return pl.ds(pl.multiple_of(64 * n, 64), 64)

    def u_sum(level, tag):
        for j in range(1, NZ):
            to = up(j)
            rcopy(sty.at[level, piece(to)], uwr.at[level, j - 1], (tag,), dev(y, to, x, c)).start()

    def u_total(level, tag):
        recv(uwr.at[level], (tag,), d_up)
        total = sty[level, piece(z), :].astype(F32)
        for j in range(1, NZ):
            total = total + uwr[level, j - 1].astype(F32)
        us[level] = total.astype(BF)

    def half_sum():
        for j in range(1, NZ):
            to = up(j)
            rcopy(sty.at[2, piece(to)], uwl.at[z - 4], ("u0",), dev(y, to, x, c)).start()

    def half_total():
        @pl.when(z < 4)
        def _():
            recv(uwl, ("u0",), d_up)

        @pl.when(z >= 4)
        def _():
            uwl[z - 4] = sty[2, piece(z), :]
            recv(uwl.at[pl.ds(0, 3)], ("u0",), d_up)

        us2[...] = sum(uwl[i].astype(F32) for i in range(4))


    for d in (1, 0):
        for h in range(HH):
            st[d, head(h), :] = mm(weighted(h, 2 + d), gb[h], TN).astype(BF)

    place4 = lax.rem(z, 4)

    @pl.when(place4 == 3)
    def _():
        for h in range(HH):
            rcopy(st.at[1, head(h)], dch.at[head(h)], ("d", h), d_dn).start()
        rcopy(st.at[0], dnear, ("d0",), d_dn).start()

    def chain(level):
        for h in range(HH):
            recv(dch.at[head(h)], ("d", h), d_dn)
            total = dch[head(h), :].astype(F32) + st[level, head(h), :].astype(F32)
            dsum[head(h), :] = total.astype(BF)
            rcopy(dsum.at[head(h)], dch.at[head(h)], ("d", h), d_dn).start()

    class Scatter:
        def __init__(self, tag, own, bu, bd, pu, pd):
            self.tag, self.own = tag, own
            self.side = {"u": (bu, pu, d_up), "d": (bd, pd, d_dn)}

        def step(self, k, h, way):
            first = (h < 2) == (way == "u")
            assert k > 0 or first
            buf, got, device = self.side[way]
            value = self.own(up(4 - k) if way == "u" else up(k - 4), h)
            if k > 1 or (k == 1 and first):
                recv(got.at[k - 1, head(h)], (self.tag, way, k - 1, h), device)
                value = value + got[k - 1, head(h), :].astype(F32)
            buf[k, head(h), :] = value.astype(BF)
            send(buf.at[k, head(h)], got.at[k, head(h)], (self.tag, way, k, h), device)

        def start(self, i):
            for h in (2 * i, 2 * i + 1):
                self.step(0, h, "ud"[i])
                self.step(1, h, "du"[i])

        def wave(self, i, k):
            for h in (2 * i, 2 * i + 1):
                self.step(k, h, "ud"[i])
                if k < 3:
                    self.step(k + 1, h, "du"[i])

        def final(self, h):
            total = self.own(z, h)
            for way in ("u", "d"):
                _, got, device = self.side[way]
                recv(got.at[3, head(h)], (self.tag, way, 3, h), device)
                total = total + got[3, head(h), :].astype(F32)
            return total

    for i in (0, 1):
        bb[0, i] = gf[y * 2 + i]

    for h in range(HH):
        ag_recv(3, h)
        total = sb[0, head(h), :].astype(F32)
        for n in range(1, NZ):
            total = total + sb[n, head(h), :].astype(F32)
        tsend[head(h), :] = total.astype(BF)

        @pl.when((y == 0) | (y == 2))
        def _(h=h):
            rcopy(tsend.at[head(h)], trecv.at[0, head(h)], ("t", h), d_y[1]).start()

        @pl.when(y == 1)
        def _(h=h):
            rcopy(tsend.at[head(h)], trecv.at[0, head(h)], ("t", h), d_y[3]).start()

    @pl.when(y > 0)
    def _():
        u_sum(main, "u1")

    @pl.when(y == 3)
    def _():
        u_sum(0, "u2")

    @pl.when(z >= 4)
    def _():
        half_sum()

    for h in range(HH):
        db[h] = (mm(gb[h], vb[h], NT) * weight(h)).astype(BF)
        dq_o[pl.ds(h, 128, stride=HH), :] = mm(db[h], kb[h])
        dk_o[pl.ds(h, 128, stride=HH), :] = mm(db[h], qb[h], TN)
        dv_o[pl.ds(h, 128, stride=HH), :] = mm(pb[h], gb[h], TN)

    @pl.when(y < 2)
    def _():
        for h in range(HH):
            recv(trecv.at[0, head(h)], ("t", h), d_y[1])
            both = tsend[head(h), :].astype(F32) + trecv[0, head(h), :].astype(F32)
            tsum[head(h), :] = both.astype(BF)

            @pl.when(y == 1)
            def _(h=h):
                rcopy(tsum.at[head(h)], trecv.at[1, head(h)], ("tt", h), d_y[1]).start()

            @pl.when(y == 0)
            def _(h=h):
                rcopy(tsum.at[head(h)], trecv.at[1, head(h)], ("tt", h), d_y[3]).start()

    z1 = z + 1 - 2 * lax.rem(z, 2)
    zp = lax.div(z, 2)
    zp1 = 2 * (zp + 1 - 2 * lax.rem(zp, 2))
    zq1 = 4 * (1 - lax.div(z, 4))
    b0 = lax.rem(z, 2).astype(F32)
    b1 = lax.rem(zp, 2).astype(F32)
    b2 = lax.div(z, 4).astype(F32)

    def from_states(h, states, levels, bits):
        block = jnp.concatenate(states, axis=0)
        wide = jnp.concatenate(states, axis=1)
        qw, gw = [], []
        for l, bit in zip(levels, bits):
            scale = lam(l, h) if bit is None else lam(l, h) * bit
            qw.append((qb[h].astype(F32) * scale).astype(BF))
            gw.append((gb[h].astype(F32) * scale).astype(BF))
        attf[h] += mm(jnp.concatenate(qw, axis=1), block)
        place = pl.ds(h, 128, stride=HH)
        dq_o[place, :] = dq_o[place, :] + mm(jnp.concatenate(gw, axis=1), wide, NT)

    for h in range(HH):
        pair = (sb[zp1, head(h), :].astype(F32) + sb[zp1 + 1, head(h), :].astype(F32)).astype(BF)
        quad = sb[zq1, head(h), :].astype(F32)
        for i in range(1, 4):
            quad = quad + sb[zq1 + i, head(h), :].astype(F32)
        from_states(h, [sb[z1, head(h), :], pair, quad.astype(BF)], (2, 3, 4), (b0, b1, b2))

    for j in (1, 3, 2):
        recv(bb.at[j, c], ("b", j), d_y[j])
        send(bb.at[j, c], bb.at[j, c], ("b2",), d_sib)

    @pl.when(place4 == 2)
    def _():
        chain(1)

    @pl.when(y == 0)
    def _():
        trecv[...] = jnp.zeros_like(trecv)

    @pl.when(y == 1)
    def _():
        trecv[1] = jnp.zeros_like(tsend)

    @pl.when(y == 2)
    def _():
        trecv[0] = jnp.zeros_like(tsend)

    for h in range(HH):

        @pl.when(y == 3)
        def _(h=h):
            recv(trecv.at[0, head(h)], ("t", h), d_y[1])

        @pl.when(y >= 2)
        def _(h=h):
            recv(trecv.at[1, head(h)], ("tt", h), d_y[1])

        from_states(h, [trecv[0, head(h), :], trecv[1, head(h), :]], (5, 6), (None, None))
        a16 = attf[h].astype(BF)
        att16[:, 128 * h : 128 * h + 128] = a16
        at[0, head(h), :] = a16.T
        for j in (1, 3, 2):
            send(at.at[0, head(h)], at.at[j, head(h)], ("at", h), d_y[j])

    @pl.when(place4 == 1)
    def _():
        chain(0)

    def m_part(index):
        cols = pl.ds(pl.multiple_of(index * 512, 512), 512)
        return mm(att16[...], wo[:, cols]).astype(BF)

    for i in range(NX):
        mp[0, i] = m_part(i * 2 + sib)
    send(mp.at[0], mr, ("m",), d_sib)
    for i in range(NX):
        mp[1, i] = m_part(i * 2 + c)

    def own_c(zd, h):
        return cf[zd, head(h), :]

    rs_c = Scatter("c", own_c, cu, cd, xu, xd)

    def product(i):
        part = pl.ds(HALF * i, HALF)
        for h in (2 * i, 2 * i + 1):
            recv(at.at[pl.ds(1, 3), head(h)], ("at", h), d_y[1])
        a = jnp.concatenate([at[n, part, :] for n in range(NY)], axis=1)
        for n in range(4):
            b = jnp.concatenate(
                [bb[m, n // 2, :, 256 * (n % 2) : 256 * (n % 2) + 256] for m in range(NY)], axis=0
            )
            out = mm(a, b)
            cf[2 * n, part, :] = out[:, :128]
            cf[2 * n + 1, part, :] = out[:, 128:]
        rs_c.start(i)

    recv(bb.at[pl.ds(1, 3), sib], ("b2",), d_sib)
    product(0)

    def u_send(j, level):
        rcopy(us.at[level], ur.at[j - 1], ("u%dy" % j,), d_y[4 - j]).start()

    @pl.when(y > 0)
    def _():
        u_total(main, "u1")

    @pl.when(y == 1)
    def _():
        u_send(1, 0)

    @pl.when(y == 2)
    def _():
        u_send(1, 1)
        u_send(2, 1)

    @pl.when(y == 3)
    def _():
        u_send(2, 1)
        u_send(3, 1)

    product(1)
    recv(mr, ("m",), d_sib)
    for j in (1, 3, 2):
        ms[j - 1] = (mp[1, xp(j)].astype(F32) + mr[xp(j)].astype(F32)).astype(BF)
        send(ms.at[j - 1], mx.at[j - 1], ("mx",), d_x[j])
    rs_c.wave(0, 1)

    @pl.when(y == 3)
    def _():
        u_total(0, "u2")
        u_send(1, 0)

    half_total()

    rs_c.wave(1, 1)

    def later_all():
        usum[...] = jnp.zeros_like(usum)
        for j in (1, 2, 3):

            @pl.when(y + j < NY)
            def _(j=j):
                recv(ur.at[j - 1], ("u%dy" % j,), d_y[4 - j])
                usum[...] += ur[j - 1].astype(F32)

        uo[0] = usum[...].astype(BF)
        uo[1] = (usum[...] + us2[...]).astype(BF)
        uall[NZ - 1] = uo[jnp.where(z < 4, 1, 0)]
        for j in range(1, NZ):
            to = up(j)

            @pl.when((y < 3) | (to < 4))
            def _(j=j, to=to):
                low = jnp.where(to < 4, 1, 0)
                rcopy(uo.at[low], uall.at[j - 1], ("ua",), dev(y, to, x, c)).start()

    later_all()
    rs_c.wave(0, 2)
    rs_c.wave(1, 2)
    rs_c.wave(0, 3)
    rs_c.wave(1, 3)

    out = mp[1, x].astype(F32) + mr[x].astype(F32)
    recv(mx, ("mx",), d_x[1])
    for j in (1, 3, 2):
        out = out + mx[j - 1].astype(F32)
    mixed_o[...] = out.astype(BF)

    some = (y < 3) | (z < 4)

    @pl.when(some)
    def _():
        recv(uall.at[pl.ds(0, NZ - 1)], ("ua",), d_up)

    @pl.when(jnp.logical_not(some))
    def _():
        uall[...] = jnp.zeros_like(uall)

    @pl.when(place4 == 0)
    def _():
        for h in range(HH):
            recv(dch.at[head(h)], ("d", h), d_dn)
        dfin[...] = dch[...]

    @pl.when(place4 == 1)
    def _():
        dfin[...] = dch[...]

    @pl.when(place4 == 2)
    def _():
        recv(dnear, ("d0",), d_dn)
        dfin[...] = dnear[...]

    @pl.when(place4 == 3)
    def _():
        dfin[...] = jnp.zeros_like(dfin)

    for h in range(HH):
        own_slots = [lax.rem(z - 2 * h - i + 2 * NZ - 1, NZ) for i in (0, 1)]
        later = jnp.concatenate([uall[n] for n in own_slots], axis=0).astype(F32)
        block = (dfin[head(h), :].astype(F32) + later).astype(BF)
        place = pl.ds(h, 128, stride=HH)
        dk_o[place, :] = dk_o[place, :] + mm(vb[h], block, NT)
        dv_o[place, :] = dv_o[place, :] + mm(kb[h], block)

    for h in (0, 1, 2, 3):
        pg_o[head(h), :] = rs_c.final(h)

    for name, ref in (
        ("og", gf.at[pl.ds(0, 4)]), ("og2", gf.at[pl.ds(0, 3)]), ("b", gf.at[pl.ds(0, 3)]),
        ("b2", gf.at[pl.ds(0, 3)]), ("ag", sb.at[pl.ds(0, 7)]),
        ("c", sb.at[pl.ds(0, 7)]), ("at", at.at[pl.ds(0, 3)]), ("m", mr), ("mx", mx),
    ):
        assert group[name] == math.prod(ref.shape), (name, group[name])
        sent(ref, name)

    @pl.when(y > 0)
    def _():
        sent(uwr.at[0], "u1")

    @pl.when(y == 3)
    def _():
        sent(uwr.at[0], "u2")

    @pl.when(y < 3)
    def _():
        sent(uwr.at[0], "ua")

    @pl.when((y == 3) & (z < 4))
    def _():
        sent(uwl.at[pl.ds(0, 3)], "ua")

    @pl.when((y == 3) & (z >= 4))
    def _():
        sent(uwl, "ua")

    @pl.when(z >= 4)
    def _():
        sent(uwr.at[0], "u0")

    @pl.when(place4 > 0)
    def _():
        sent(dch, "d")

    @pl.when(place4 == 3)
    def _():
        sent(dnear, "d0")

    @pl.when(y < 3)
    def _():
        sent(tsend, "t")

    @pl.when(y < 2)
    def _():
        sent(tsend, "tt")

    for j in (1, 2, 3):

        @pl.when(y >= j)
        def _(j=j):
            sent(us.at[0], "u%dy" % j)

    assert len(sids.table) <= S_SEM and len(ids.table) <= N_SEM, (len(sids.table), len(ids.table))


N_SEM = 97
S_SEM = 21
VLIM = 28


def out_kernel(*refs):
    src, dst, sem = refs[:5], refs[5:10], refs[10]
    copies = [pltpu.make_async_copy(a, b, sem.at[i]) for i, (a, b) in enumerate(zip(src, dst))]
    for op in copies:
        op.start()
    for op in copies:
        op.wait()


def body(queries, keys, values, level_weights, out_proj, out_grad):
    def flat(a):
        return a.reshape(512, 128)

    any_spec = pl.BlockSpec(memory_space=pl.ANY)
    blk = (512, 128)
    v = pltpu.VMEM
    outs = pl.pallas_call(
        body_kernel,
        out_shape=(
            jax.ShapeDtypeStruct((128, 512), BF),
            jax.ShapeDtypeStruct(blk, F32),
            jax.ShapeDtypeStruct(blk, F32),
            jax.ShapeDtypeStruct(blk, F32),
            jax.ShapeDtypeStruct(blk, F32),
        ),
        in_specs=[pl.BlockSpec(memory_space=pltpu.HBM)] * 6,
        out_specs=[pl.BlockSpec(memory_space=pltpu.VMEM)] * 5,
        scratch_shapes=[
            v(blk, F32), v(blk, F32), v(blk, F32),
            v((7, 4, 128), F32), v((32, 128), F32), v((128, 32), F32),
            v((512, 4096), BF), v((8, 128, 512), BF), v((128, 512), F32),
            v((4, 128, 128), BF), v((4, 128, 128), BF), v((4, 128, 128), BF), v((4, 128, 128), BF),
            v((4, 128, 128), BF), v((4, 128, 128), BF), v((4, 128, 128), F32), v((128, 512), BF),
            v((8, 512, 128), BF), v((2, 512, 128), BF), v((3, 512, 128), BF),
            v(blk, BF), v((2, 512, 128), BF), v(blk, BF),
            v((2, 7, 64, 128), BF), v((4, 64, 128), BF), v((2, 64, 128), BF), v((64, 128), F32), v((3, 64, 128), BF),
            v((64, 128), F32), v((2, 64, 128), BF), v((8, 64, 128), BF),
            v(blk, BF), v(blk, BF), v(blk, BF), v(blk, BF),
            v((4, 2, 128, 512), BF), v((4, 512, 128), BF), v((8, 512, 128), F32),
            v((4, 512, 128), BF), v((4, 512, 128), BF), v((4, 512, 128), BF), v((4, 512, 128), BF),
            v((2, 4, 128, 512), BF), v((4, 128, 512), BF), v((3, 128, 512), BF), v((3, 128, 512), BF),
            pltpu.SemaphoreType.DMA((6,)),
            pltpu.SemaphoreType.DMA((S_SEM,)),
            pltpu.SemaphoreType.DMA((N_SEM,)),
        ],
        compiler_params=pltpu.CompilerParams(
            collective_id=0, has_side_effects=True, vmem_limit_bytes=VLIM << 20
        ),
        name="log_linear",
    )(*[pltpu.with_memory_space_constraint(a, pltpu.HBM) for a in (flat(queries), flat(keys), flat(values), level_weights, out_proj, out_grad)])
    mixed, dq, dk, dv, pg = pl.pallas_call(
        out_kernel,
        out_shape=tuple(jax.ShapeDtypeStruct(o.shape, o.dtype) for o in outs),
        in_specs=[any_spec] * 5,
        out_specs=[any_spec] * 5,
        scratch_shapes=[pltpu.SemaphoreType.DMA((5,))],
        compiler_params=pltpu.CompilerParams(vmem_limit_bytes=4 << 20),
        name="results",
    )(*outs)
    heads = queries.shape
    return mixed, dq.reshape(heads), dk.reshape(heads), dv.reshape(heads), pg


def solution(mesh):
    placed = (
        P("seq", "head", None),
        P("seq", "head", None),
        P("seq", "head", None),
        P(None, "head", "seq"),
        P("head", None),
        P("seq", "head"),
    )
    return jax.shard_map(
        body,
        mesh=mesh,
        in_specs=placed,
        out_specs=(
            P("seq", "head"),
            P("seq", "head", None),
            P("seq", "head", None),
            P("seq", "head", None),
            P("head", "seq"),
        ),
        check_vma=False,
    )
```

```python
import functools
import math

import jax
import jax.numpy as jnp
from jax import lax
from jax.experimental import pallas as pl
from jax.experimental.pallas import tpu as pltpu
from jax.sharding import PartitionSpec as P

MESH = pl.DeviceIdType.MESH
BF = jnp.bfloat16
F32 = jnp.float32
NN = (((1,), (0,)), ((), ()))
NT = (((1,), (1,)), ((), ()))
TN = (((0,), (0,)), ((), ()))
NY, NZ, NX = 4, 8, 4
HH = 4
HALF = 256


def mm(a, b, dims=NN):
    return lax.dot_general(a, b, dims, preferred_element_type=F32)


class Ids:
    def __init__(self):
        self.table = {}

    def __call__(self, *key):
        return self.table.setdefault(key, len(self.table))


def body_kernel(
    q_h, k_h, v_h, lam_h, wo_h, og_h,
    mixed_o, dq_o, dk_o, dv_o, pg_o,
    qf, kf, vf, lam_v, lam_s, lam_t, wo, gf, gacc,
    qb, kb, vb, gb, pb, db, attf, att16,
    sb, st, sty, tsend, trecv, tsum, uwr, uwl, us, us2, ur, usum, uo, uall,
    dch, dnear, dsum, dfin,
    bb, at, cf, cu, cd, xu, xd,
    mp, mr, ms, mx,
    lsem, ssem, rsem,
):
    seq = lax.axis_index("seq")
    hd = lax.axis_index("head")
    y, z = lax.div(seq, NZ), lax.rem(seq, NZ)
    x, c = lax.div(hd, 2), lax.rem(hd, 2)
    sib = 1 - c

    def dev(yy, zz, xx, cc):
        return (yy * NZ + zz, xx * 2 + cc)

    def up(j):
        return lax.rem(z + j + NZ, NZ)

    def yp(j):
        return lax.rem(y + j + NY, NY)

    def xp(j):
        return lax.rem(x + j + NX, NX)

    d_sib = dev(y, z, x, sib)
    d_x = {j: dev(y, z, xp(j), c) for j in (1, 2, 3)}
    d_y = {j: dev(yp(j), z, x, c) for j in (1, 2, 3)}
    d_up, d_dn = dev(y, up(1), x, c), dev(y, up(-1), x, c)

    ids, sids = Ids(), Ids()
    group = {}

    def rcopy(src, dst, key, device):
        return pltpu.make_async_remote_copy(
            src_ref=src, dst_ref=dst, send_sem=ssem.at[sids(key[0])], recv_sem=rsem.at[ids(*key)],
            device_id=device, device_id_type=MESH,
        )

    def send(src, dst, key, device):
        rcopy(src, dst, key, device).start()
        group[key[0]] = group.get(key[0], 0) + math.prod(src.shape)

    def sent(ref, name):
        pltpu.make_async_remote_copy(
            src_ref=ref, dst_ref=ref, send_sem=ssem.at[sids(name)], recv_sem=rsem.at[0],
            device_id=d_sib, device_id_type=MESH,
        ).wait_send()

    def recv(dst, key, device):
        rcopy(dst, dst, key, device).wait_recv()

    loads = {}

    def load(name, src, dst):
        op = pltpu.make_async_copy(src, dst, lsem.at[len(loads)])
        op.start()
        loads[name] = op

    load("k", k_h, kf)
    load("v", v_h, vf)
    load("og", og_h, gf.at[hd])
    load("q", q_h, qf)
    load("lam", lam_h, lam_v)
    load("wo", wo_h, wo)

    barrier = pltpu.get_barrier_semaphore()
    partners = [d_sib] + [d_x[j] for j in (1, 2, 3)] + [d_y[j] for j in (1, 2, 3)] + [d_up, d_dn]
    for who in partners:
        pl.semaphore_signal(barrier, inc=1, device_id=who, device_id_type=MESH)

    def head(h):
        return pl.ds(128 * h, 128)

    def rows(ref, h):
        return ref[pl.ds(h, 128, stride=HH), :]

    loads["k"].wait()
    loads["v"].wait()
    for h in range(HH):
        kh = rows(kf, h).astype(BF)
        vh = rows(vf, h).astype(BF)
        kb[h] = kh
        vb[h] = vh
        sb[z, head(h), :] = mm(kh, vh, TN).astype(BF)

    pl.semaphore_wait(barrier, len(partners))

    for j in (1, 3, 2):
        send(og_h, gf.at[hd], ("og", j), d_x[j])

    def ag_send(k, h):
        su, sd = up(-k), up(k)
        if k < 3 or h < 2:
            send(sb.at[su, head(h)], sb.at[su, head(h)], ("ag", "u", k, h), d_up)
        if k < 3 or h >= 2:
            send(sb.at[sd, head(h)], sb.at[sd, head(h)], ("ag", "d", k, h), d_dn)

    def ag_recv(k, h):
        if k < 3 or h < 2:
            recv(sb.at[up(-k - 1), head(h)], ("ag", "u", k, h), d_up)
        if k < 3 or h >= 2:
            recv(sb.at[up(k + 1), head(h)], ("ag", "d", k, h), d_dn)

    def ag_relay(k, heads=range(HH)):
        for h in heads:
            ag_recv(k - 1, h)
            ag_send(k, h)

    for h in range(HH):
        ag_send(0, h)
    send(og_h, gf.at[hd], ("og", 0), d_sib)

    loads["q"].wait()
    loads["lam"].wait()
    lam_s[...] = jnp.zeros_like(lam_s)
    for l in range(7):
        lam_s[pl.ds(4 * l, 4), :] = lam_v[l]
    lam_t[...] = lam_s[...].T

    def lam(l, h):
        return lam_t[:, 4 * l + h : 4 * l + h + 1]

    t_pos = lax.broadcasted_iota(jnp.int32, (128, 128), 0)
    s_pos = lax.broadcasted_iota(jnp.int32, (128, 128), 1)
    causal = t_pos >= s_pos
    cross = (t_pos >= 64) & (s_pos < 64)

    def weight(h):
        return jnp.where(causal, jnp.where(cross, lam(1, h), lam(0, h)), 0.0)

    for h in range(HH):
        qh = rows(qf, h).astype(BF)
        qb[h] = qh
        probs = (mm(qh, kb[h], NT) * weight(h)).astype(BF)
        pb[h] = probs
        attf[h] = mm(probs, vb[h])

    ag_relay(1)

    loads["og"].wait()
    loads["wo"].wait()

    def g_part(index):
        cols = pl.ds(pl.multiple_of(index * 512, 512), 512)
        return mm(gf[index], wo[:, cols], NT)

    def og_relay(j):
        src = xp(-j) * 2 + c
        recv(gf.at[src], ("og", j), d_x[j])
        send(gf.at[src], gf.at[src], ("og2", j), d_sib)

    gacc[...] = g_part(hd)
    recv(gf.at[x * 2 + sib], ("og", 0), d_sib)
    gacc[...] += g_part(x * 2 + sib)
    og_relay(1)
    og_relay(3)
    ag_relay(2, (0, 1))
    og_relay(2)
    for j in (1, 2, 3):
        send(gf.at[yp(j) * 2 + c], bb.at[j, c], ("b", j), d_y[j])
    ag_relay(2, (2, 3))
    for j in (1, 3, 2):
        gacc[...] += g_part(xp(-j) * 2 + c)

    def g_far(j):
        src = xp(-j) * 2 + sib
        recv(gf.at[src], ("og2", j), d_sib)
        gacc[...] += g_part(src)

    g_far(1)
    g_far(3)
    ag_relay(3, (0, 1))
    g_far(2)
    for h in range(HH):
        gb[h] = gacc[:, 128 * h : 128 * h + 128].astype(BF)
    ag_relay(3, (2, 3))

    def weighted(h, level):
        return (qb[h].astype(F32) * lam(level, h)).astype(BF)

    for d in (4, 3, 2):
        for h in range(HH):
            sty[{3: 0, 4: 1, 2: 2}[d], head(h), :] = mm(weighted(h, 2 + d), gb[h], TN).astype(BF)
    near = lax.rem(y, 2)
    main = jnp.where(y == 1, 0, 1)

    def piece(n):
        return pl.ds(pl.multiple_of(64 * n, 64), 64)

    def u_sum(level, tag):
        for j in range(1, NZ):
            to = up(j)
            rcopy(sty.at[level, piece(to)], uwr.at[level, j - 1], (tag,), dev(y, to, x, c)).start()

    def u_total(level, tag):
        recv(uwr.at[level], (tag,), d_up)
        total = sty[level, piece(z), :].astype(F32)
        for j in range(1, NZ):
            total = total + uwr[level, j - 1].astype(F32)
        us[level] = total.astype(BF)

    def half_sum():
        for j in range(1, NZ):
            to = up(j)
            rcopy(sty.at[2, piece(to)], uwl.at[z - 4], ("u0",), dev(y, to, x, c)).start()

    def half_total():
        @pl.when(z < 4)
        def _():
            recv(uwl, ("u0",), d_up)

        @pl.when(z >= 4)
        def _():
            uwl[z - 4] = sty[2, piece(z), :]
            recv(uwl.at[pl.ds(0, 3)], ("u0",), d_up)

        us2[...] = sum(uwl[i].astype(F32) for i in range(4))


    for d in (1, 0):
        for h in range(HH):
            st[d, head(h), :] = mm(weighted(h, 2 + d), gb[h], TN).astype(BF)

    place4 = lax.rem(z, 4)

    @pl.when(place4 == 3)
    def _():
        for h in range(HH):
            rcopy(st.at[1, head(h)], dch.at[head(h)], ("d", h), d_dn).start()
        rcopy(st.at[0], dnear, ("d0",), d_dn).start()

    def chain(level):
        for h in range(HH):
            recv(dch.at[head(h)], ("d", h), d_dn)
            total = dch[head(h), :].astype(F32) + st[level, head(h), :].astype(F32)
            dsum[head(h), :] = total.astype(BF)
            rcopy(dsum.at[head(h)], dch.at[head(h)], ("d", h), d_dn).start()

    class Scatter:
        def __init__(self, tag, own, bu, bd, pu, pd):
            self.tag, self.own = tag, own
            self.side = {"u": (bu, pu, d_up), "d": (bd, pd, d_dn)}

        def step(self, k, h, way):
            first = (h < 2) == (way == "u")
            assert k > 0 or first
            buf, got, device = self.side[way]
            value = self.own(up(4 - k) if way == "u" else up(k - 4), h)
            if k > 1 or (k == 1 and first):
                recv(got.at[k - 1, head(h)], (self.tag, way, k - 1, h), device)
                value = value + got[k - 1, head(h), :].astype(F32)
            buf[k, head(h), :] = value.astype(BF)
            send(buf.at[k, head(h)], got.at[k, head(h)], (self.tag, way, k, h), device)

        def start(self, i):
            for h in (2 * i, 2 * i + 1):
                self.step(0, h, "ud"[i])
                self.step(1, h, "du"[i])

        def wave(self, i, k):
            for h in (2 * i, 2 * i + 1):
                self.step(k, h, "ud"[i])
                if k < 3:
                    self.step(k + 1, h, "du"[i])

        def final(self, h):
            total = self.own(z, h)
            for way in ("u", "d"):
                _, got, device = self.side[way]
                recv(got.at[3, head(h)], (self.tag, way, 3, h), device)
                total = total + got[3, head(h), :].astype(F32)
            return total

    for i in (0, 1):
        bb[0, i] = gf[y * 2 + i]

    for h in range(HH):
        ag_recv(3, h)
        total = sb[0, head(h), :].astype(F32)
        for n in range(1, NZ):
            total = total + sb[n, head(h), :].astype(F32)
        tsend[head(h), :] = total.astype(BF)

        @pl.when((y == 0) | (y == 2))
        def _(h=h):
            rcopy(tsend.at[head(h)], trecv.at[0, head(h)], ("t", h), d_y[1]).start()

        @pl.when(y == 1)
        def _(h=h):
            rcopy(tsend.at[head(h)], trecv.at[0, head(h)], ("t", h), d_y[3]).start()

    @pl.when(y > 0)
    def _():
        u_sum(main, "u1")

    @pl.when(y == 3)
    def _():
        u_sum(0, "u2")

    @pl.when(z >= 4)
    def _():
        half_sum()

    for h in range(HH):
        db[h] = (mm(gb[h], vb[h], NT) * weight(h)).astype(BF)
        dq_o[pl.ds(h, 128, stride=HH), :] = mm(db[h], kb[h])
        dk_o[pl.ds(h, 128, stride=HH), :] = mm(db[h], qb[h], TN)
        dv_o[pl.ds(h, 128, stride=HH), :] = mm(pb[h], gb[h], TN)

    @pl.when(y < 2)
    def _():
        for h in range(HH):
            recv(trecv.at[0, head(h)], ("t", h), d_y[1])
            both = tsend[head(h), :].astype(F32) + trecv[0, head(h), :].astype(F32)
            tsum[head(h), :] = both.astype(BF)

            @pl.when(y == 1)
            def _(h=h):
                rcopy(tsum.at[head(h)], trecv.at[1, head(h)], ("tt", h), d_y[1]).start()

            @pl.when(y == 0)
            def _(h=h):
                rcopy(tsum.at[head(h)], trecv.at[1, head(h)], ("tt", h), d_y[3]).start()

    z1 = z + 1 - 2 * lax.rem(z, 2)
    zp = lax.div(z, 2)
    zp1 = 2 * (zp + 1 - 2 * lax.rem(zp, 2))
    zq1 = 4 * (1 - lax.div(z, 4))
    b0 = lax.rem(z, 2).astype(F32)
    b1 = lax.rem(zp, 2).astype(F32)
    b2 = lax.div(z, 4).astype(F32)

    def from_states(h, states, levels, bits):
        block = jnp.concatenate(states, axis=0)
        wide = jnp.concatenate(states, axis=1)
        qw, gw = [], []
        for l, bit in zip(levels, bits):
            scale = lam(l, h) if bit is None else lam(l, h) * bit
            qw.append((qb[h].astype(F32) * scale).astype(BF))
            gw.append((gb[h].astype(F32) * scale).astype(BF))
        attf[h] += mm(jnp.concatenate(qw, axis=1), block)
        place = pl.ds(h, 128, stride=HH)
        dq_o[place, :] = dq_o[place, :] + mm(jnp.concatenate(gw, axis=1), wide, NT)

    for h in range(HH):
        pair = (sb[zp1, head(h), :].astype(F32) + sb[zp1 + 1, head(h), :].astype(F32)).astype(BF)
        quad = sb[zq1, head(h), :].astype(F32)
        for i in range(1, 4):
            quad = quad + sb[zq1 + i, head(h), :].astype(F32)
        from_states(h, [sb[z1, head(h), :], pair, quad.astype(BF)], (2, 3, 4), (b0, b1, b2))

    for j in (1, 3, 2):
        recv(bb.at[j, c], ("b", j), d_y[j])
        send(bb.at[j, c], bb.at[j, c], ("b2",), d_sib)

    @pl.when(place4 == 2)
    def _():
        chain(1)

    @pl.when(y == 0)
    def _():
        trecv[...] = jnp.zeros_like(trecv)

    @pl.when(y == 1)
    def _():
        trecv[1] = jnp.zeros_like(tsend)

    @pl.when(y == 2)
    def _():
        trecv[0] = jnp.zeros_like(tsend)

    for h in range(HH):

        @pl.when(y == 3)
        def _(h=h):
            recv(trecv.at[0, head(h)], ("t", h), d_y[1])

        @pl.when(y >= 2)
        def _(h=h):
            recv(trecv.at[1, head(h)], ("tt", h), d_y[1])

        from_states(h, [trecv[0, head(h), :], trecv[1, head(h), :]], (5, 6), (None, None))
        a16 = attf[h].astype(BF)
        att16[:, 128 * h : 128 * h + 128] = a16
        at[0, head(h), :] = a16.T
        for j in (2, 1, 3):
            send(at.at[0, head(h)], at.at[j, head(h)], ("at", h), d_y[j])

    @pl.when(place4 == 1)
    def _():
        chain(0)

    def m_part(index):
        cols = pl.ds(pl.multiple_of(index * 512, 512), 512)
        return mm(att16[...], wo[:, cols]).astype(BF)

    for i in range(NX):
        mp[0, i] = m_part(i * 2 + sib)
    send(mp.at[0], mr, ("m",), d_sib)
    for i in range(NX):
        mp[1, i] = m_part(i * 2 + c)

    def own_c(zd, h):
        return cf[zd, head(h), :]

    rs_c = Scatter("c", own_c, cu, cd, xu, xd)

    def product(i):
        part = pl.ds(HALF * i, HALF)
        for h in (2 * i, 2 * i + 1):
            recv(at.at[pl.ds(1, 3), head(h)], ("at", h), d_y[1])
        a = jnp.concatenate([at[n, part, :] for n in range(NY)], axis=1)
        for n in range(4):
            b = jnp.concatenate(
                [bb[m, n // 2, :, 256 * (n % 2) : 256 * (n % 2) + 256] for m in range(NY)], axis=0
            )
            out = mm(a, b)
            cf[2 * n, part, :] = out[:, :128]
            cf[2 * n + 1, part, :] = out[:, 128:]
        rs_c.start(i)

    recv(bb.at[pl.ds(1, 3), sib], ("b2",), d_sib)
    product(0)

    def u_send(j, level):
        rcopy(us.at[level], ur.at[j - 1], ("u%dy" % j,), d_y[4 - j]).start()

    @pl.when(y > 0)
    def _():
        u_total(main, "u1")

    @pl.when(y == 1)
    def _():
        u_send(1, 0)

    @pl.when(y == 2)
    def _():
        u_send(1, 1)
        u_send(2, 1)

    @pl.when(y == 3)
    def _():
        u_send(2, 1)
        u_send(3, 1)

    product(1)
    recv(mr, ("m",), d_sib)
    for j in (1, 3, 2):
        ms[j - 1] = (mp[1, xp(j)].astype(F32) + mr[xp(j)].astype(F32)).astype(BF)
        send(ms.at[j - 1], mx.at[j - 1], ("mx",), d_x[j])
    rs_c.wave(0, 1)

    @pl.when(y == 3)
    def _():
        u_total(0, "u2")
        u_send(1, 0)

    half_total()

    rs_c.wave(1, 1)

    def later_all():
        usum[...] = jnp.zeros_like(usum)
        for j in (1, 2, 3):

            @pl.when(y + j < NY)
            def _(j=j):
                recv(ur.at[j - 1], ("u%dy" % j,), d_y[4 - j])
                usum[...] += ur[j - 1].astype(F32)

        uo[0] = usum[...].astype(BF)
        uo[1] = (usum[...] + us2[...]).astype(BF)
        uall[NZ - 1] = uo[jnp.where(z < 4, 1, 0)]
        for j in range(1, NZ):
            to = up(j)

            @pl.when((y < 3) | (to < 4))
            def _(j=j, to=to):
                low = jnp.where(to < 4, 1, 0)
                rcopy(uo.at[low], uall.at[j - 1], ("ua",), dev(y, to, x, c)).start()

    later_all()
    rs_c.wave(0, 2)
    rs_c.wave(1, 2)
    rs_c.wave(0, 3)
    rs_c.wave(1, 3)

    out = mp[1, x].astype(F32) + mr[x].astype(F32)
    recv(mx, ("mx",), d_x[1])
    for j in (1, 3, 2):
        out = out + mx[j - 1].astype(F32)
    mixed_o[...] = out.astype(BF)

    some = (y < 3) | (z < 4)

    @pl.when(some)
    def _():
        recv(uall.at[pl.ds(0, NZ - 1)], ("ua",), d_up)

    @pl.when(jnp.logical_not(some))
    def _():
        uall[...] = jnp.zeros_like(uall)

    @pl.when(place4 == 0)
    def _():
        for h in range(HH):
            recv(dch.at[head(h)], ("d", h), d_dn)
        dfin[...] = dch[...]

    @pl.when(place4 == 1)
    def _():
        dfin[...] = dch[...]

    @pl.when(place4 == 2)
    def _():
        recv(dnear, ("d0",), d_dn)
        dfin[...] = dnear[...]

    @pl.when(place4 == 3)
    def _():
        dfin[...] = jnp.zeros_like(dfin)

    for h in range(HH):
        own_slots = [lax.rem(z - 2 * h - i + 2 * NZ - 1, NZ) for i in (0, 1)]
        later = jnp.concatenate([uall[n] for n in own_slots], axis=0).astype(F32)
        block = (dfin[head(h), :].astype(F32) + later).astype(BF)
        place = pl.ds(h, 128, stride=HH)
        dk_o[place, :] = dk_o[place, :] + mm(vb[h], block, NT)
        dv_o[place, :] = dv_o[place, :] + mm(kb[h], block)

    for h in (0, 1, 2, 3):
        pg_o[head(h), :] = rs_c.final(h)

    for name, ref in (
        ("og", gf.at[pl.ds(0, 4)]), ("og2", gf.at[pl.ds(0, 3)]), ("b", gf.at[pl.ds(0, 3)]),
        ("b2", gf.at[pl.ds(0, 3)]), ("ag", sb.at[pl.ds(0, 7)]),
        ("c", sb.at[pl.ds(0, 7)]), ("at", at.at[pl.ds(0, 3)]), ("m", mr), ("mx", mx),
    ):
        assert group[name] == math.prod(ref.shape), (name, group[name])
        sent(ref, name)

    @pl.when(y > 0)
    def _():
        sent(uwr.at[0], "u1")

    @pl.when(y == 3)
    def _():
        sent(uwr.at[0], "u2")

    @pl.when(y < 3)
    def _():
        sent(uwr.at[0], "ua")

    @pl.when((y == 3) & (z < 4))
    def _():
        sent(uwl.at[pl.ds(0, 3)], "ua")

    @pl.when((y == 3) & (z >= 4))
    def _():
        sent(uwl, "ua")

    @pl.when(z >= 4)
    def _():
        sent(uwr.at[0], "u0")

    @pl.when(place4 > 0)
    def _():
        sent(dch, "d")

    @pl.when(place4 == 3)
    def _():
        sent(dnear, "d0")

    @pl.when(y < 3)
    def _():
        sent(tsend, "t")

    @pl.when(y < 2)
    def _():
        sent(tsend, "tt")

    for j in (1, 2, 3):

        @pl.when(y >= j)
        def _(j=j):
            sent(us.at[0], "u%dy" % j)

    assert len(sids.table) <= S_SEM and len(ids.table) <= N_SEM, (len(sids.table), len(ids.table))


N_SEM = 97
S_SEM = 21
VLIM = 28


def out_kernel(*refs):
    src, dst, sem = refs[:5], refs[5:10], refs[10]
    copies = [pltpu.make_async_copy(a, b, sem.at[i]) for i, (a, b) in enumerate(zip(src, dst))]
    for op in copies:
        op.start()
    for op in copies:
        op.wait()


def body(queries, keys, values, level_weights, out_proj, out_grad):
    def flat(a):
        return a.reshape(512, 128)

    any_spec = pl.BlockSpec(memory_space=pl.ANY)
    blk = (512, 128)
    v = pltpu.VMEM
    outs = pl.pallas_call(
        body_kernel,
        out_shape=(
            jax.ShapeDtypeStruct((128, 512), BF),
            jax.ShapeDtypeStruct(blk, F32),
            jax.ShapeDtypeStruct(blk, F32),
            jax.ShapeDtypeStruct(blk, F32),
            jax.ShapeDtypeStruct(blk, F32),
        ),
        in_specs=[pl.BlockSpec(memory_space=pltpu.HBM)] * 6,
        out_specs=[pl.BlockSpec(memory_space=pltpu.VMEM)] * 5,
        scratch_shapes=[
            v(blk, F32), v(blk, F32), v(blk, F32),
            v((7, 4, 128), F32), v((32, 128), F32), v((128, 32), F32),
            v((512, 4096), BF), v((8, 128, 512), BF), v((128, 512), F32),
            v((4, 128, 128), BF), v((4, 128, 128), BF), v((4, 128, 128), BF), v((4, 128, 128), BF),
            v((4, 128, 128), BF), v((4, 128, 128), BF), v((4, 128, 128), F32), v((128, 512), BF),
            v((8, 512, 128), BF), v((2, 512, 128), BF), v((3, 512, 128), BF),
            v(blk, BF), v((2, 512, 128), BF), v(blk, BF),
            v((2, 7, 64, 128), BF), v((4, 64, 128), BF), v((2, 64, 128), BF), v((64, 128), F32), v((3, 64, 128), BF),
            v((64, 128), F32), v((2, 64, 128), BF), v((8, 64, 128), BF),
            v(blk, BF), v(blk, BF), v(blk, BF), v(blk, BF),
            v((4, 2, 128, 512), BF), v((4, 512, 128), BF), v((8, 512, 128), F32),
            v((4, 512, 128), BF), v((4, 512, 128), BF), v((4, 512, 128), BF), v((4, 512, 128), BF),
            v((2, 4, 128, 512), BF), v((4, 128, 512), BF), v((3, 128, 512), BF), v((3, 128, 512), BF),
            pltpu.SemaphoreType.DMA((6,)),
            pltpu.SemaphoreType.DMA((S_SEM,)),
            pltpu.SemaphoreType.DMA((N_SEM,)),
        ],
        compiler_params=pltpu.CompilerParams(
            collective_id=0, has_side_effects=True, vmem_limit_bytes=VLIM << 20
        ),
        name="log_linear",
    )(*[pltpu.with_memory_space_constraint(a, pltpu.HBM) for a in (flat(queries), flat(keys), flat(values), level_weights, out_proj, out_grad)])
    mixed, dq, dk, dv, pg = pl.pallas_call(
        out_kernel,
        out_shape=tuple(jax.ShapeDtypeStruct(o.shape, o.dtype) for o in outs),
        in_specs=[any_spec] * 5,
        out_specs=[any_spec] * 5,
        scratch_shapes=[pltpu.SemaphoreType.DMA((5,))],
        compiler_params=pltpu.CompilerParams(vmem_limit_bytes=4 << 20),
        name="results",
    )(*outs)
    heads = queries.shape
    return mixed, dq.reshape(heads), dk.reshape(heads), dv.reshape(heads), pg


def solution(mesh):
    placed = (
        P("seq", "head", None),
        P("seq", "head", None),
        P("seq", "head", None),
        P(None, "head", "seq"),
        P("head", None),
        P("seq", "head"),
    )
    return jax.shard_map(
        body,
        mesh=mesh,
        in_specs=placed,
        out_specs=(
            P("seq", "head"),
            P("seq", "head", None),
            P("seq", "head", None),
            P("seq", "head", None),
            P("head", "seq"),
        ),
        check_vma=False,
    )
```
